32 devices in a mesh: groups: 2 (over y), sky: 4 (over z), epoch: 2 (over x), band: 2 (over core).
Axes of the slice: x: 2, y: 2, z: 4, core: 2. Of those that a mesh axis runs over, the one named last changes fastest.
Arguments:
- slot_pixels: bfloat16 [96, 6, 32, 512], P(('groups', 'sky', 'epoch'), 'band'), parts along dimension 0, may hold values from -6 to 6
- slot_tile: int32 [96, 1], P(('groups', 'sky', 'epoch')), parts along dimension 0, may hold values from 0 to 3; in each aligned block of 6 rows (0 to 5, 6 to 11, ...) at most 2 rows name the same one
- slot_offset: int32 [96, 2], P(('groups', 'sky', 'epoch')), parts along dimension 0, may hold values from -5 to 5
- slot_frac: bfloat16 [96, 2], P(('groups', 'sky', 'epoch')), parts along dimension 0, may hold values from 0.049804688 to 0.94921875
- slot_sigma: bfloat16 [96, 6], P(('groups', 'sky', 'epoch'), 'band'), parts along dimension 0, may hold values from 0.5 to 2
- clip_mask: int32 [96, 6, 16], P(('groups', 'sky', 'epoch')), parts along dimension 0, may hold values 0 or 1
- slot_count: int32 [16], P(('groups', 'sky', 'epoch')), parts along dimension 0, may hold values from 4 to 6
- template: bfloat16 [6, 256, 512], P('band', ('groups', 'sky')), parts along dimension 1, may hold values from -6 to 6
- prior_weight: float32 [6, 256], P('band', ('groups', 'sky')), parts along dimension 1, may hold values from 0.5 to 4
Outputs:
- coadd_image: bfloat16 [6, 256, 512], P('band', ('groups', 'sky'), 'epoch'), parts along dimension 1
- depth_norm: bfloat16 [6, 256, 512], P('band', ('groups', 'sky'), 'epoch'), parts along dimension 1
The draws below stay inside these ranges and needn't reach their ends.
There are 2 independent parts, one for each index of `groups`. The reference program is written for one: setup_inputs(seed, part) draws one part's arguments, and reference() takes and returns one part's arrays. A program takes and returns all parts, laid end to end along the dimension named above; each array names one. Nothing has to cross between parts.
Inputs may be any that keep to these rules, and one draw needn't show every extreme that they name: `slot_tile`: among the 6 rows of one reading device no owner is named more than 2 times, a bound that some block reaches. `slot_count`: slots of a reading device at or after its count are padding.
All inputs are finite; a program needn't handle non-finite values. No bound on the sum of `clip_mask` on one device may be relied on, other than what follows from the above.
Results may differ from the reference program's by a relative error of at most 0.014.
Values may be sent and summed in bfloat16 or wider, within the bound.
A program may use at most 64 MiB of HBM per device.

```python
import math
import jax
import jax.numpy as jnp
import numpy as np
from jax import lax

BAND_COUNT = 6
TILE_COLS = 512
ROWS_DEV = 32
MAX_SHIFT = 5
MARGIN = 8
CAPACITY = 2
SLOT_DEV = 6
SLOT_TOTAL = 48
PATCH_ROWS = 128
N_SKY = 4
N_EPOCH = 2


def plant(array, key, least, high):
    longest = array.shape.index(max(array.shape))
    spots = []
    for shift in (0, 1):
        where = [jax.random.randint(jax.random.fold_in(key, axis), (), 0, length) for axis, length in enumerate(array.shape)]
        where[longest] = (where[longest] + shift) % array.shape[longest]
        spots.append(tuple(where))
    return array.at[spots[0]].set(least).at[spots[1]].set(high)


def block_levels(own_key, extent, shards, smallest, high):
    level = 1.0
    for position, parts in shards:
        steps = jax.random.uniform(jax.random.fold_in(jax.random.fold_in(own_key, 6), position), (parts,), jnp.float32, smallest / len(shards), high / len(shards))
        level = level * jnp.repeat(jnp.exp(steps), extent[position] // parts).reshape((-1,) + (1,) * (len(extent) - 1 - position))
    return level


def shared_out(stream_key, own, number, rows, amount, top, most, skew):
    sequence = jax.random.permutation(stream_key, amount)
    heavy_load, usual = portions_of(amount, rows * top, most, skew, True), portions_of(amount, rows * top, most, skew, False)
    places = jnp.arange(amount)

    def named(lengths, offset_by):
        used = int((lengths > 0).sum())
        fixed = max(1, used // 4)
        moved = fixed + (places - fixed + offset_by * (used - fixed)) % max(1, amount - fixed)
        return jnp.zeros((amount,), jnp.int32).at[sequence[jnp.where(places < fixed, places, moved)]].set(jnp.asarray(lengths, jnp.int32))

    lengths = jnp.where(number % 4 == 0, named(heavy_load, number // 4), named(usual, number - number // 4 - 1))
    mixed = jax.random.permutation(jax.random.fold_in(own, 3), amount)
    giver, receiver = mixed[0:amount // 2 * 2:2], mixed[1:amount // 2 * 2:2]
    slack = jnp.minimum(lengths[giver] - 1, most - lengths[receiver]) // 2
    slack = jnp.where((giver == sequence[0]) | (receiver == sequence[0]) | (lengths[receiver] == 0), 0, jnp.maximum(slack, 0))
    moved = jax.random.randint(jax.random.fold_in(own, 4), (amount // 2,), 0, 1 << 20) % (slack + 1)
    lengths = lengths.at[giver].add(-moved).at[receiver].add(moved)
    labels = jnp.searchsorted(jnp.cumsum(lengths), jnp.arange(rows * top), side="right").astype(jnp.int32)
    table = labels.reshape(top, rows).T
    table = table[jax.random.permutation(jax.random.fold_in(own, 1), rows)]
    offset_by = jax.random.randint(jax.random.fold_in(own, 2), (rows, 1), 0, top)
    return jnp.take_along_axis(table, (jnp.arange(top)[None, :] + offset_by) % top, axis=1)


def portions_of(amount, total, reach, lean, full):
    loads = [(1 << 20) // math.isqrt(standing ** lean) + 1 for standing in range(1, amount + 1)]
    largest = reach if full else min(reach, max(-(-total // amount), total * loads[0] // sum(loads)))
    least = 1 if total - largest >= amount - 1 else 0
    counts, spare = [largest] + [least] * (amount - 1), total - largest - least * (amount - 1)
    while spare > 0:
        movable = [i for i in range(1, amount) if counts[i] < largest] or [i for i in range(1, amount) if counts[i] < reach]
        pool, left = sum([loads[i] for i in movable]), spare
        for i in movable:
            more = min(reach - counts[i], max(1, left * loads[i] // pool), spare)
            counts[i] = counts[i] + more
            spare = spare - more
    return np.array(counts)


def gaussian(rng, dims, spread, most, cuts=(), kind=jnp.bfloat16):
    result = spread * jax.random.normal(rng, dims, jnp.float32)
    if cuts:
        result = result * block_levels(rng, dims, cuts, -0.22, 0.18)
    return jnp.clip(result, -most, most).astype(kind)


def setup_inputs(seed: int = 0, part: int = 0) -> dict:
    splits = jax.random.split(jax.random.key(seed), 10)
    part_splits = jax.random.split(jax.random.fold_in(splits[9], part), 10)
    slot_pixels = gaussian(part_splits[0], (SLOT_TOTAL, BAND_COUNT, ROWS_DEV, TILE_COLS), 1.0, 6.0, ((0, 8), (1, 2)))
    slot_tile_keys = jax.random.split(jax.random.fold_in(part_splits[1], 1), SLOT_TOTAL // SLOT_DEV)
    slot_tile_turns = jax.random.permutation(jax.random.fold_in(part_splits[1], 3), SLOT_TOTAL // SLOT_DEV)
    slot_tile = jax.vmap(lambda own, number: shared_out(jax.random.fold_in(part_splits[1], 2), own, number, SLOT_DEV, N_SKY, 1, CAPACITY, 2))(slot_tile_keys, slot_tile_turns).reshape((SLOT_TOTAL, 1))
    slot_offset = plant(jax.random.randint(part_splits[2], (SLOT_TOTAL, 2), 0 - MAX_SHIFT, MAX_SHIFT + 1), jax.random.fold_in(part_splits[2], 1), 0 - MAX_SHIFT, MAX_SHIFT).astype(jnp.int32)
    slot_frac = jnp.clip(0.049804688 + 0.89941406 * jax.random.uniform(part_splits[3], (SLOT_TOTAL, 2), jnp.float32) ** block_levels(part_splits[3], (SLOT_TOTAL, 2), ((0, 8),), -0.2, 0.2), 0.049804688, 0.94921875).astype(jnp.bfloat16)
    slot_sigma = jnp.clip(jnp.exp(math.log(2.0) - 1.3862944 * jax.random.uniform(part_splits[4], (SLOT_TOTAL, BAND_COUNT), jnp.float32) ** block_levels(part_splits[4], (SLOT_TOTAL, BAND_COUNT), ((0, 8), (1, 2)), -0.2, 0.2)), 0.5, 2.0).astype(jnp.bfloat16)
    clip_mask = plant((jax.random.randint(part_splits[5], (SLOT_TOTAL, (ROWS_DEV + 2 * MARGIN) // 8, TILE_COLS // 32), 0, 8) < 7).astype(jnp.int32), jax.random.fold_in(part_splits[5], 1), 0, 1)
    slot_count = plant(jax.random.randint(part_splits[6], (N_SKY * N_EPOCH,), 3 * SLOT_DEV // 4, SLOT_DEV + 1), jax.random.fold_in(part_splits[6], 1), 3 * SLOT_DEV // 4, SLOT_DEV).astype(jnp.int32)
    template = gaussian(part_splits[7], (BAND_COUNT, PATCH_ROWS, TILE_COLS), 1.0, 6.0, ((0, 2), (1, 4)))
    prior_weight = jnp.clip(jnp.exp(math.log(4.0) - 2.0794415 * jax.random.uniform(part_splits[8], (BAND_COUNT, PATCH_ROWS), jnp.float32) ** block_levels(part_splits[8], (BAND_COUNT, PATCH_ROWS), ((0, 2), (1, 4)), -0.2, 0.2)), 0.5, 4.0)
    return {"slot_pixels": slot_pixels, "slot_tile": slot_tile, "slot_offset": slot_offset, "slot_frac": slot_frac, "slot_sigma": slot_sigma, "clip_mask": clip_mask, "slot_count": slot_count, "template": template, "prior_weight": prior_weight}


CLIP_WIDTH = 3.0


def lanczos(distance):
    inside = jnp.abs(distance) < 3.0
    return jnp.where(inside, jnp.sinc(distance) * jnp.sinc(distance / 3.0), 0.0)


def tap_weights(fraction):
    steps_back = jnp.arange(-3, 3, dtype=jnp.int32)
    distance = (-steps_back).astype(jnp.float32) - fraction
    rounded = lanczos(distance).astype(jnp.bfloat16)
    return lax.optimization_barrier(rounded).astype(jnp.float32)


def reference(slot_pixels, slot_tile, slot_offset, slot_frac, slot_sigma, clip_mask, slot_count, template, prior_weight):
    slot_number = slot_pixels.shape[0]
    canvas_rows = ROWS_DEV + 2 * MARGIN
    patch_rows = template.shape[1]
    tile_cols = template.shape[2]
    template_pad = jnp.pad(template.astype(jnp.float32), ((0, 0), (MARGIN, MARGIN), (0, 0)))
    empty_sums = jnp.zeros((BAND_COUNT, patch_rows + 2 * MARGIN, tile_cols), jnp.float32)
    row_index = jnp.arange(canvas_rows, dtype=jnp.int32)
    col_index = jnp.arange(tile_cols, dtype=jnp.int32)

    def one_slot(carried, slot_index):
        flux_sums, weight_sums = carried
        pixels = lax.dynamic_index_in_dim(slot_pixels, slot_index, 0, keepdims=False).astype(jnp.float32)
        tile_index = slot_tile[slot_index, 0]
        shift_y = slot_offset[slot_index, 0]
        shift_x = slot_offset[slot_index, 1]
        taps_y = tap_weights(slot_frac[slot_index, 0].astype(jnp.float32))
        taps_x = tap_weights(slot_frac[slot_index, 1].astype(jnp.float32))
        is_live = ((slot_index % SLOT_DEV) < slot_count[slot_index // SLOT_DEV]).astype(jnp.float32)
        padded = jnp.pad(pixels, ((0, 0), (0, 0), (MARGIN, MARGIN)))
        columns = jnp.zeros((BAND_COUNT, ROWS_DEV, tile_cols), jnp.float32)
        col_cover = jnp.zeros((tile_cols,), jnp.float32)
        for tap_index in range(6):
            step_back = tap_index - 3
            shifted = lax.dynamic_slice_in_dim(padded, MARGIN - shift_x + step_back, tile_cols, 2)
            columns = columns + taps_x[tap_index] * shifted
            source_col = col_index - shift_x + step_back
            inside = (source_col >= 0) & (source_col < tile_cols)
            col_cover = col_cover + jnp.where(inside, taps_x[tap_index], 0.0)
        columns = lax.optimization_barrier(columns.astype(jnp.bfloat16)).astype(jnp.float32)
        column_pad = jnp.pad(columns, ((0, 0), (2 * MARGIN, 2 * MARGIN), (0, 0)))
        warped = jnp.zeros((BAND_COUNT, canvas_rows, tile_cols), jnp.float32)
        row_cover = jnp.zeros((canvas_rows,), jnp.float32)
        for tap_index in range(6):
            step_back = tap_index - 3
            shifted = lax.dynamic_slice_in_dim(column_pad, MARGIN - shift_y + step_back, canvas_rows, 1)
            warped = warped + taps_y[tap_index] * shifted
            source_row = row_index - MARGIN - shift_y + step_back
            inside = (source_row >= 0) & (source_row < ROWS_DEV)
            row_cover = row_cover + jnp.where(inside, taps_y[tap_index], 0.0)
        row_cover = jnp.clip(row_cover, 0.0, 1.0)
        col_cover = jnp.clip(col_cover, 0.0, 1.0)
        block_mask = clip_mask[slot_index].astype(jnp.float32)
        expanded = jnp.repeat(jnp.repeat(block_mask, 8, axis=0), 32, axis=1) * is_live
        plane = (expanded * row_cover[:, None]) * col_cover[None, :]
        sigmas = slot_sigma[slot_index].astype(jnp.float32)
        weight = plane[None] / (sigmas * sigmas)[:, None, None]
        framed = lax.dynamic_slice_in_dim(template_pad, tile_index * ROWS_DEV, canvas_rows, 1)
        scale = CLIP_WIDTH * sigmas[:, None, None]
        clipped = framed + scale * jnp.tanh((warped - framed) / scale)
        start = tile_index * ROWS_DEV
        old_flux = lax.dynamic_slice_in_dim(flux_sums, start, canvas_rows, 1)
        old_weight = lax.dynamic_slice_in_dim(weight_sums, start, canvas_rows, 1)
        flux_sums = lax.dynamic_update_slice_in_dim(flux_sums, old_flux + weight * clipped, start, 1)
        weight_sums = lax.dynamic_update_slice_in_dim(weight_sums, old_weight + weight, start, 1)
        return (flux_sums, weight_sums), None

    (flux_sums, weight_sums), _ = lax.scan(one_slot, (empty_sums, empty_sums), jnp.arange(slot_number, dtype=jnp.int32))
    flux_sum = flux_sums[:, MARGIN:MARGIN + patch_rows]
    weight_sum = weight_sums[:, MARGIN:MARGIN + patch_rows]
    prior = prior_weight[:, :, None]
    coadd_image = ((flux_sum + prior * template.astype(jnp.float32)) / (weight_sum + prior)).astype(jnp.bfloat16)
    depth_map = weight_sum + prior
    band_mean = jnp.sum(depth_map, axis=(1, 2)) / (patch_rows * tile_cols)
    depth_norm = (depth_map / band_mean[:, None, None]).astype(jnp.bfloat16)
    return coadd_image, depth_norm
```

```python
import functools
import math

import jax
import jax.numpy as jnp
from jax import lax
from jax.experimental import pallas as pl
from jax.experimental.pallas import tpu as pltpu
from jax.sharding import PartitionSpec as P

MARGIN = 8
BLOCK_ROWS = 8
REACH = 3
TAPS = 2 * REACH
LANES = 128
CAPACITY = 2
CLIP_WIDTH = 3.0
NOBODY = -64.0
PRIOR_LANE = 64
AT_ONCE = 4
TILE, DY, DX, FY, FX, SIGMA = range(6)
MESH = pl.DeviceIdType.MESH
F32 = jnp.float32
BF16 = jnp.bfloat16


def sinc(x):
    at_zero = x == 0.0
    turned = math.pi * jnp.where(at_zero, 1.0, x)
    return jnp.where(at_zero, 1.0, jnp.sin(turned) / turned)


def lanczos(distance):
    inside = jnp.abs(distance) < 3.0
    return jnp.where(inside, sinc(distance) * sinc(distance / 3.0), 0.0)


def rounded(x):
    return x.astype(BF16).astype(F32)


def iota(shape, dim):
    return lax.broadcasted_iota(jnp.int32, shape, dim)


def ones_where(condition):
    return jnp.where(condition, 1.0, 0.0).astype(BF16)


def dot(a, b):
    return jnp.dot(a, b, preferred_element_type=F32)


def dot_first(a, b):
    return lax.dot_general(a, b, (((0,), (0,)), ((), ())), preferred_element_type=F32)


def between(x, extent):
    return (x >= 0.0) & (x < float(extent))


def coadd_kernel(
    shape, steer_ref, count_ref, tile_ref, offset_ref, frac_ref, sigma_ref, mask_ref,
    template_ref, prior_ref, pixels_ref,
    coadd_ref, depth_ref,
    pixels, small, group, others, tap_table, columns, columns_held, template_held,
    framed, flux, left, weigh, inverse, warped, send, held, cover_ref,
    local_sem, group_sem, others_sem, template_sem, columns_sem, flux_sem,
):
    bands, sky, epochs, rows, cols, slots, blocks, mask_cols = shape
    part = cols // epochs
    canvas = rows + 2 * MARGIN
    padded = cols + LANES
    held_slots = slots + -slots % 8
    fields = SIGMA + bands
    field_at = blocks * mask_cols
    at_once = sky if sky <= AT_ONCE else 1
    pairs = at_once * CAPACITY
    me = lax.axis_index("sky")
    epoch = lax.axis_index("epoch")
    own_cols = pl.ds(pl.multiple_of(epoch * part, LANES), part)

    def sky_peer(d):
        return lax.rem(me + d, sky)

    def epoch_peer(d):
        return lax.rem(epoch + d, epochs)

    barrier = pltpu.get_barrier_semaphore()
    for d in range(1, sky):
        pl.semaphore_signal(barrier, inc=1, device_id={"sky": sky_peer(d)}, device_id_type=MESH)
    for d in range(1, epochs):
        pl.semaphore_signal(barrier, inc=1, device_id={"epoch": epoch_peer(d)}, device_id_type=MESH)
    loads = []
    for b in range(bands):
        load = pltpu.make_async_copy(pixels_ref.at[:, b], pixels.at[b], local_sem.at[b])
        load.start()
        loads.append(load)

    def remote(src, dst, sems, index, where):
        copy = pltpu.make_async_remote_copy(
            src_ref=src, dst_ref=dst, send_sem=sems.at[(0,) + index], recv_sem=sems.at[(1,) + index],
            device_id=where, device_id_type=MESH,
        )
        copy.start()
        return copy

    lane = iota((8, LANES), 1)
    small[...] = jnp.ones_like(small)
    tile = jnp.where(iota((1, slots), 1) < count_ref[0], tile_ref[...].astype(F32), NOBODY)
    small[TILE : TILE + 1] = jnp.full((1, LANES), NOBODY, F32)
    small[TILE : TILE + 1, :slots] = tile
    small[DY : DX + 1, :slots] = offset_ref[...].astype(F32)
    small[FY : FX + 1, :slots] = frac_ref[...].astype(F32)
    small[SIGMA:fields, :slots] = sigma_ref[...].astype(F32)
    by_lane = small[...]
    field_rows = by_lane.shape[0]
    place = ones_where(iota((16, LANES), 1) == iota((16, LANES), 0) + field_at)
    tall = jnp.concatenate([by_lane, jnp.zeros((16 - field_rows, LANES), F32)], 0) if field_rows < 16 else by_lane
    by_slot = dot_first(tall.astype(BF16), place[: tall.shape[0]])[:held_slots]
    cells = []
    for p in range(held_slots):
        if p < slots:
            cells.append(mask_ref[p].astype(F32))
            if blocks % 8:
                cells.append(jnp.zeros((-blocks % 8, mask_cols), F32))
        else:
            cells.append(jnp.zeros((blocks + -blocks % 8, mask_cols), F32))
    cells = jnp.concatenate(cells, 0)
    tall_blocks = blocks + -blocks % 8
    wide = (mask_cols, LANES)
    spread = ones_where((lax.rem(iota(wide, 1), mask_cols) == iota(wide, 0)) & (iota(wide, 1) < field_at))
    wide = dot(cells.astype(BF16), spread)
    wide = jnp.where(iota(wide.shape, 1) // mask_cols == lax.rem(iota(wide.shape, 0), tall_blocks), wide, 0.0)
    gather = (held_slots, held_slots * tall_blocks)
    by_slot = by_slot + dot(ones_where(iota(gather, 1) // tall_blocks == iota(gather, 0)), wide.astype(BF16))
    prior = jnp.concatenate([prior_ref[...], jnp.zeros((-bands % 8, rows), F32)], 0)
    prior = jnp.sum(prior, 1, keepdims=True)
    high = rounded(prior)
    middle = rounded(prior - high)
    by_lane = jnp.where(lane == PRIOR_LANE, high, by_lane)
    by_lane = jnp.where(lane == PRIOR_LANE + 1, middle, by_lane)
    by_lane = jnp.where(lane == PRIOR_LANE + 2, prior - high - middle, by_lane)
    group[0] = jnp.concatenate([by_slot, by_lane], 0).astype(BF16)

    def column(a, f):
        return a[:, field_at + f : field_at + f + 1]

    def slot_taps(a):
        at = iota(a.shape, 1)
        fraction = jnp.where(at < 8, column(a, FX), column(a, FY))
        return rounded(lanczos((REACH - lax.rem(at, 8)).astype(F32) - fraction))

    def column_cover(a, taps, first, width):
        at = (iota((a.shape[0], width), 1) + first).astype(F32) - column(a, DX)
        total = jnp.zeros(at.shape, F32)
        for t in range(TAPS):
            total = total + jnp.where(between(at + float(t - REACH), cols), taps[:, t : t + 1], 0.0)
        return jnp.clip(total, 0.0, 1.0)

    taps = slot_taps(by_slot)
    for t in range(TAPS):
        tap_table[t] = jnp.broadcast_to(taps[:, t : t + 1], (held_slots, LANES))

    def warp_columns(b):
        def one_slot(p, carry):
            source = jnp.concatenate([pixels[b, p].astype(F32), jnp.zeros((rows, LANES), F32)], 1)
            base = pltpu.roll(source, lax.rem(steer_ref[1, p] + padded, padded), 1)

            def tap(t):
                return jnp.concatenate([tap_table[t, pl.ds(p, 1)]] * (padded // LANES), 1)

            summed = tap(REACH) * base
            for t in range(TAPS):
                if t != REACH:
                    summed = summed + tap(t) * pltpu.roll(base, (REACH - t) % padded, 1)
            at = pl.ds(pl.multiple_of(p * rows, rows), rows)
            for e in range(epochs):
                columns[e, b, at] = summed[:, e * part : (e + 1) * part].astype(BF16)
            return carry

        lax.fori_loop(0, slots, one_slot, 0, unroll=slots <= 8)

    started = []
    columns_copies, template_copies, group_copies, others_copies, flux_copies = {}, {}, {}, {}, {}
    for b in range(bands):
        loads[b].wait()
        warp_columns(b)
        if b == 0:
            pl.semaphore_wait(barrier, sky - 1 + epochs - 1)
            for d in range(1, epochs):
                group_copies[d] = remote(
                    group.at[0], group.at[d], group_sem, (d - 1,), {"epoch": epoch_peer(d)}
                )
        for d in range(1, sky):
            template_copies[d, b] = remote(
                template_ref.at[b, :, own_cols], template_held.at[d - 1, b], template_sem, (d - 1, b),
                {"sky": sky_peer(d)},
            )
        for d in range(1, epochs):
            columns_copies[d, b] = remote(
                columns.at[epoch_peer(d), b], columns_held.at[d - 1, b], columns_sem, (d - 1, b),
                {"epoch": epoch_peer(d)},
            )

    flux[...] = jnp.zeros_like(flux)
    edge = jnp.zeros((bands, MARGIN, part), F32)
    framed[:, :MARGIN] = edge
    framed[:, MARGIN + sky * rows :] = edge
    own_rows = pl.ds(pl.multiple_of(MARGIN + me * rows, 8), rows)
    for b in range(bands):
        framed[b, own_rows] = template_ref[b, :, own_cols].astype(F32)

    depth_k = slots * rows
    cell_k = blocks * held_slots
    to_rows = ones_where(iota((LANES, depth_k), 1) // rows == iota((LANES, depth_k), 0))
    to_cells = (LANES, cell_k)
    to_cells = ones_where(
        (lax.rem(iota(to_cells, 1), held_slots) == iota(to_cells, 0)) & (iota(to_cells, 0) < slots)
    )

    def prepare(d, first_owner):
        message = group[d].astype(F32)
        a, by_lane = message[:held_slots], message[held_slots:]
        lanes = iota((held_slots, LANES), 1)
        same = (column(a, TILE) == by_lane[TILE : TILE + 1]) & (iota(lanes.shape, 0) < lanes)
        rank = jnp.sum(jnp.where(same, 1.0, 0.0), 0, keepdims=True)
        tap_rows = (REACH - iota((8, LANES), 0)).astype(F32) - by_lane[FY : FY + 1]
        tap_rows = rounded(lanczos(tap_rows))
        stack = jnp.concatenate(
            [tap_rows, jnp.broadcast_to(rank, (8, LANES)), by_lane] + [tap_rows] * (by_lane.shape[0] // 8 % 2), 0
        ).astype(BF16)
        k_stack = dot(stack, to_rows)
        gap = iota((canvas, depth_k), 0) - MARGIN - lax.rem(iota((canvas, depth_k), 1), rows)
        gap = gap.astype(F32) - k_stack[16 + DY : 17 + DY]
        row_table = jnp.zeros((canvas, depth_k), F32)
        for t in range(TAPS):
            row_table = row_table + jnp.where(gap == float(REACH - t), k_stack[t : t + 1], 0.0)
        c_stack = dot(stack, to_cells)
        c_lane = iota((canvas, cell_k), 1)
        reach = (iota((canvas, cell_k), 0) - MARGIN).astype(F32) - c_stack[16 + DY : 17 + DY]
        cover = jnp.zeros((canvas, cell_k), F32)
        for t in range(TAPS):
            cover = cover + jnp.where(between(reach + float(t - REACH), rows), c_stack[t : t + 1], 0.0)
        cover = jnp.clip(cover, 0.0, 1.0)
        cover = jnp.where(iota((canvas, cell_k), 0) // BLOCK_ROWS == c_lane // held_slots, cover, 0.0)
        cover = jnp.where(lax.rem(c_lane, held_slots) < slots, cover, 0.0)
        slot_cover = column_cover(a, slot_taps(a), epoch * part, part)
        chosen = [jnp.where(iota(a.shape, 1) // mask_cols == i, a, 0.0) for i in range(blocks)]
        wide = (LANES, part)
        spread = lax.rem(iota(wide, 0), mask_cols) == (iota(wide, 1) + epoch * part) // (cols // mask_cols)
        spread = ones_where(spread & (iota(wide, 0) < field_at))
        cells = dot(jnp.concatenate(chosen, 0).astype(BF16), spread)
        cells = (cells * jnp.concatenate([slot_cover] * blocks, 0)).astype(BF16)

        def here(stacked, owner, k):
            return (stacked[16 + TILE : 17 + TILE] == owner.astype(F32)) & (stacked[8:9] == float(k))

        pair_row = iota((pairs, LANES), 0)
        picked = (by_lane[TILE : TILE + 1] == (first_owner + pair_row // CAPACITY).astype(F32)) & (
            rank == lax.rem(pair_row, CAPACITY).astype(F32)
        ) & (iota((pairs, LANES), 1) < slots)
        for b in range(bands):
            scale = 1.0 / (CLIP_WIDTH * by_lane[SIGMA + b : SIGMA + b + 1])
            scale = jnp.sum(jnp.where(picked, scale, 0.0), 1, keepdims=True)
            inverse[d, b] = jnp.broadcast_to(scale, (pairs, LANES))
        sigma = [c_stack[16 + SIGMA + b : 17 + SIGMA + b] for b in range(bands)]
        weight = [cover * (CLIP_WIDTH / jnp.where(s > 0.0, s, 1.0)) for s in sigma]
        lhs = [[] for _ in range(bands)]
        for pair in range(pairs):
            owner, k = jnp.int32(first_owner + pair // CAPACITY), pair % CAPACITY
            at = slice(pair * canvas, (pair + 1) * canvas)
            left[d, at] = jnp.where(here(k_stack, owner, k), row_table, 0.0).astype(BF16)
            mine = here(c_stack, owner, k)
            for b in range(bands):
                lhs[b].append(jnp.where(mine, weight[b], 0.0))
        for b in range(bands):
            weigh[d, b] = dot(jnp.concatenate(lhs[b], 0).astype(BF16), cells)

    def process(d, b, first_owner):
        source = columns[epoch, b] if d == 0 else columns_held[d - 1, b]
        warped[...] = dot(left[d], source)
        for o in range(at_once):
            at = pl.ds(pl.multiple_of((first_owner + o) * rows, 8), canvas)
            frame = framed[b, at]
            total = flux[b, at]
            for k in range(CAPACITY):
                pair = o * CAPACITY + k
                here = slice(pair * canvas, (pair + 1) * canvas)
                scale = jnp.concatenate([inverse[d, b, pair : pair + 1]] * (part // LANES), 1)
                total = total + weigh[d, b, here] * jnp.tanh((warped[here] - frame) * scale)
            flux[b, at] = total

    def all_owners(step):
        if sky == at_once:
            step(0)
        else:
            lax.fori_loop(0, sky // at_once, lambda i, c: (step(i * at_once), c)[1], 0)

    for d in range(1, epochs):
        group_copies[d].wait_recv()
    for d in range(1, sky):
        others_copies[d] = remote(group, others.at[d - 1], others_sem, (d - 1,), {"sky": sky_peer(d)})
    if sky == at_once:
        for d in range(epochs):
            prepare(d, 0)
    for b in range(bands):
        for d in range(1, sky):
            template_copies[d, b].wait_recv()
            at = pl.ds(pl.multiple_of(MARGIN + lax.rem(me - d + sky, sky) * rows, 8), rows)
            framed[b, at] = template_held[d - 1, b].astype(F32)
        for d in range(epochs):
            if d:
                columns_copies[d, b].wait_recv()

            def step(first_owner, d=d, b=b):
                if sky != at_once:
                    prepare(d, first_owner)
                process(d, b, first_owner)

            all_owners(step)
        for d in range(1, sky):
            at = pl.ds(pl.multiple_of(MARGIN + sky_peer(d) * rows, 8), rows)
            send[d - 1, b] = flux[b, at].astype(BF16)
            flux_copies[d, b] = remote(
                send.at[d - 1, b], held.at[d - 1, b], flux_sem, (d - 1, b), {"sky": sky_peer(d)}
            )

    for d in range(1, sky):
        others_copies[d].wait_recv()
    square = (LANES, LANES)
    by_block = iota(square, 0) // BLOCK_ROWS == iota(square, 1) // mask_cols
    by_block = ones_where(by_block & (iota(square, 0) < canvas) & (iota(square, 1) < field_at))
    wide = (cols, LANES)
    by_cell = ones_where(iota(wide, 0) // (cols // mask_cols) == lax.rem(iota(wide, 1), mask_cols))
    wide = (LANES, part)
    to_cols = lax.rem(iota(wide, 0), mask_cols) == (iota(wide, 1) + epoch * part) // (cols // mask_cols)
    to_cols = ones_where(to_cols)

    def depth_from(groups):
        messages = [message[e] for message in groups for e in range(epochs)]
        every = jnp.concatenate([m[:held_slots].astype(F32) for m in messages], 0)
        prior_total = jnp.zeros((8, 1), F32)
        for message in messages[::epochs]:
            message = message[held_slots : held_slots + 8].astype(F32)
            prior_total = prior_total + jnp.sum(message[:, PRIOR_LANE : PRIOR_LANE + 3], 1, keepdims=True)
        number = every.shape[0]
        taps = slot_taps(every)
        cover = cover_ref.at[:number]
        cover[...] = column_cover(every, taps, 0, cols)
        at = iota((number, LANES), 1)

        def row_cover(row):
            total = jnp.zeros(row.shape, F32)
            for t in range(TAPS):
                total = total + jnp.where(between(row + float(t - REACH), rows), taps[:, 8 + t : 9 + t], 0.0)
            return jnp.clip(total, 0.0, 1.0)

        tile = column(every, TILE)
        row = (at - MARGIN).astype(F32)
        canvas_cover = row_cover(row - column(every, DY))
        in_patch = between(row + tile * float(rows), sky * rows) & (at < canvas)
        canvas_cover = jnp.where(in_patch, canvas_cover, 0.0)
        area = dot(canvas_cover.astype(BF16), by_block) * dot(cover[...].astype(BF16), by_cell)
        area = jnp.where(at < field_at, every * area, 0.0)
        area = jnp.sum(area, 1, keepdims=True)
        precision = [1.0 / (column(every, SIGMA + b) * column(every, SIGMA + b)) for b in range(bands)]
        totals = []
        for b in range(bands):
            total = jnp.sum(area * jnp.where(tile >= 0.0, precision[b], 0.0), 0, keepdims=True)
            totals.append(total + prior_total[b : b + 1] * float(cols))
        group_rows = rows // BLOCK_ROWS
        wide = (number, bands * rows)
        in_band = iota(wide, 1)
        row = (lax.rem(in_band, rows) + me * rows).astype(F32) - tile * float(rows) - column(every, DY)
        profile = row_cover(row)
        factor = jnp.zeros(wide, F32)
        for b in range(bands):
            factor = jnp.where(in_band // rows == b, precision[b], factor)
        profile = profile * factor
        block = lax.rem(in_band, rows) // BLOCK_ROWS
        lhs = jnp.concatenate([jnp.where(block == g, profile, 0.0) for g in range(group_rows)], 0).astype(BF16)
        first = MARGIN // BLOCK_ROWS
        canvas_block = (first + group_rows * me).astype(F32) - tile * float(group_rows)
        chosen = [
            jnp.where(((at // mask_cols).astype(F32) == canvas_block + float(g)) & (at < field_at), every, 0.0)
            for g in range(group_rows)
        ]
        cells = dot(jnp.concatenate(chosen, 0).astype(BF16), to_cols)
        own_cover = cover[:, own_cols]
        cells = (cells * jnp.concatenate([own_cover] * group_rows, 0)).astype(BF16)
        return (dot_first(lhs, cells), *totals)

    if sky <= AT_ONCE:
        weights, *totals = depth_from([group[...]] + [others[d - 1] for d in range(1, sky)])
    else:
        weights, *totals = lax.fori_loop(
            0, sky - 1,
            lambda d, sums: tuple(x + y for x, y in zip(sums, depth_from([others[d]]))),
            depth_from([group[...]]),
        )
    means = [total * (1.0 / (sky * rows * cols)) for total in totals]
    diagonal = iota((rows, rows), 0) == iota((rows, rows), 1)
    depths = []
    for b in range(bands):
        prior = jnp.sum(jnp.where(diagonal, prior_ref[b : b + 1], 0.0), 1, keepdims=True)
        depth = weights[b * rows : (b + 1) * rows] + prior
        depth_ref[b] = (depth / means[b]).astype(BF16)
        depths.append(depth)
    for b in range(bands):
        total = flux[b, own_rows]
        for d in range(1, sky):
            flux_copies[d, b].wait_recv()
            total = total + held[d - 1, b].astype(F32)
        coadd_ref[b] = (framed[b, own_rows] + total / depths[b]).astype(BF16)
    for copies in (group_copies, others_copies, template_copies, columns_copies, flux_copies):
        for copy in copies.values():
            copy.wait_send()


def on_device(
    slot_pixels, slot_tile, slot_offset, slot_frac, slot_sigma, clip_mask, slot_count, template, prior_weight
):
    sky = lax.axis_size("sky")
    epochs = lax.axis_size("epoch")
    slots, bands, rows, cols = slot_pixels.shape
    blocks, mask_cols = clip_mask.shape[1:]
    part = cols // epochs
    canvas = rows + 2 * MARGIN
    held_slots = slots + -slots % 8
    field_rows = SIGMA + bands + -(SIGMA + bands) % 8
    message = held_slots + field_rows
    at_once = sky if sky <= AT_ONCE else 1
    pairs = at_once * CAPACITY
    vmem = pl.BlockSpec(memory_space=pltpu.VMEM)
    smem = pl.BlockSpec(memory_space=pltpu.SMEM)
    block = jax.ShapeDtypeStruct((bands, rows, part), BF16)
    patch = sky * rows + 2 * MARGIN
    return pl.pallas_call(
        functools.partial(coadd_kernel, (bands, sky, epochs, rows, cols, slots, blocks, mask_cols)),
        out_shape=(block, block),
        in_specs=[smem] * 2 + [vmem] * 7 + [pl.BlockSpec(memory_space=pl.ANY)],
        out_specs=(vmem, vmem),
        scratch_shapes=[
            pltpu.VMEM((bands, slots, rows, cols), BF16),
            pltpu.VMEM((field_rows, LANES), F32),
            pltpu.VMEM((epochs, message, LANES), BF16),
            pltpu.VMEM((sky - 1, epochs, message, LANES), BF16),
            pltpu.VMEM((TAPS, held_slots, LANES), F32),
            pltpu.VMEM((epochs, bands, slots * rows, part), BF16),
            pltpu.VMEM((epochs - 1, bands, slots * rows, part), BF16),
            pltpu.VMEM((sky - 1, bands, rows, part), BF16),
            pltpu.VMEM((bands, patch, part), F32),
            pltpu.VMEM((bands, patch, part), F32),
            pltpu.VMEM((epochs, pairs * canvas, slots * rows), BF16),
            pltpu.VMEM((epochs, bands, pairs * canvas, part), F32),
            pltpu.VMEM((epochs, bands, pairs, LANES), F32),
            pltpu.VMEM((pairs * canvas, part), F32),
            pltpu.VMEM((sky - 1, bands, rows, part), BF16),
            pltpu.VMEM((sky - 1, bands, rows, part), BF16),
            pltpu.VMEM(((sky if sky <= AT_ONCE else 1) * epochs * held_slots, cols), F32),
            pltpu.SemaphoreType.DMA((bands,)),
            pltpu.SemaphoreType.DMA((2, epochs - 1)),
            pltpu.SemaphoreType.DMA((2, sky - 1)),
            pltpu.SemaphoreType.DMA((2, sky - 1, bands)),
            pltpu.SemaphoreType.DMA((2, epochs - 1, bands)),
            pltpu.SemaphoreType.DMA((2, sky - 1, bands)),
        ],
        compiler_params=pltpu.CompilerParams(collective_id=0, has_side_effects=True),
        name="coadd",
    )(
        slot_offset.T, slot_count, slot_tile.T, slot_offset.T, slot_frac.T, slot_sigma.T, clip_mask,
        template, prior_weight, slot_pixels,
    )


def solution(mesh):
    in_specs = (
        P(("groups", "sky", "epoch"), "band", None, None),
        P(("groups", "sky", "epoch"), None),
        P(("groups", "sky", "epoch"), None),
        P(("groups", "sky", "epoch"), None),
        P(("groups", "sky", "epoch"), "band"),
        P(("groups", "sky", "epoch"), None, None),
        P(("groups", "sky", "epoch")),
        P("band", ("groups", "sky"), None),
        P("band", ("groups", "sky")),
    )
    out_specs = (P("band", ("groups", "sky"), "epoch"), P("band", ("groups", "sky"), "epoch"))
    return jax.shard_map(
        on_device, mesh=mesh, in_specs=in_specs, out_specs=out_specs, check_vma=False
    )
```

```python
import functools
import math

import jax
import jax.numpy as jnp
from jax import lax
from jax.experimental import pallas as pl
from jax.experimental.pallas import tpu as pltpu
from jax.sharding import PartitionSpec as P

MARGIN = 8
BLOCK_ROWS = 8
REACH = 3
TAPS = 2 * REACH
LANES = 128
CAPACITY = 2
CLIP_WIDTH = 3.0
NOBODY = -64.0
PRIOR_LANE = 64
AT_ONCE = 4
TILE, DY, DX, FY, FX, SIGMA = range(6)
MESH = pl.DeviceIdType.MESH
F32 = jnp.float32
BF16 = jnp.bfloat16


def sinc(x):
    at_zero = x == 0.0
    turned = math.pi * jnp.where(at_zero, 1.0, x)
    return jnp.where(at_zero, 1.0, jnp.sin(turned) / turned)


def lanczos(distance):
    inside = jnp.abs(distance) < 3.0
    return jnp.where(inside, sinc(distance) * sinc(distance / 3.0), 0.0)


def rounded(x):
    return x.astype(BF16).astype(F32)


def iota(shape, dim):
    return lax.broadcasted_iota(jnp.int32, shape, dim)


def ones_where(condition):
    return jnp.where(condition, 1.0, 0.0).astype(BF16)


def dot(a, b):
    return jnp.dot(a, b, preferred_element_type=F32)


def dot_first(a, b):
    return lax.dot_general(a, b, (((0,), (0,)), ((), ())), preferred_element_type=F32)


def between(x, extent):
    return (x >= 0.0) & (x < float(extent))


def coadd_kernel(
    shape, *refs,
):
    count_ref, *inputs = refs[:9]
    (
        coadd_ref, depth_ref,
        offset_ref, frac_ref, template_ref, tile_ref, sigma_ref, mask_ref, prior_ref,
        pixels, small, group, others, tap_table, lag_ref, kernel_x, columns, columns_held, template_held,
        framed, flux, left, weigh, inverse, warped, send, held, cover_ref,
        local_sem, group_sem, others_sem, template_sem, columns_sem, flux_sem,
    ) = refs[9:]
    bands, sky, epochs, rows, cols, slots, blocks, mask_cols = shape
    part = cols // epochs
    canvas = rows + 2 * MARGIN
    padded = cols + LANES
    held_slots = slots + -slots % 8
    fields = SIGMA + bands
    field_at = blocks * mask_cols
    at_once = sky if sky <= AT_ONCE else 1
    pairs = at_once * CAPACITY
    me = lax.axis_index("sky")
    epoch = lax.axis_index("epoch")
    own_cols = pl.ds(pl.multiple_of(epoch * part, LANES), part)

    def sky_peer(d):
        return lax.rem(me + d, sky)

    def epoch_peer(d):
        return lax.rem(epoch + d, epochs)

    barrier = pltpu.get_barrier_semaphore()
    for d in range(1, sky):
        pl.semaphore_signal(barrier, inc=1, device_id={"sky": sky_peer(d)}, device_id_type=MESH)
    for d in range(1, epochs):
        pl.semaphore_signal(barrier, inc=1, device_id={"epoch": epoch_peer(d)}, device_id_type=MESH)
    targets = [offset_ref, frac_ref] + [pixels.at[b] for b in range(bands)] + [
        template_ref, tile_ref, sigma_ref, mask_ref, prior_ref
    ]
    sources = inputs[:2] + [inputs[2].at[:, b] for b in range(bands)] + inputs[3:]
    loads = []
    for i, (source, target) in enumerate(zip(sources, targets)):
        loads.append(pltpu.make_async_copy(source, target, local_sem.at[i]))
        loads[-1].start()
    pixel_loads, loads = loads[2 : 2 + bands], loads[:2] + loads[2 + bands :]

    def remote(src, dst, sems, index, where):
        copy = pltpu.make_async_remote_copy(
            src_ref=src, dst_ref=dst, send_sem=sems.at[(0,) + index], recv_sem=sems.at[(1,) + index],
            device_id=where, device_id_type=MESH,
        )
        copy.start()
        return copy

    tall = (2 * LANES, LANES)
    reached = LANES + 2 * MARGIN
    source_at = jnp.where(iota(tall, 0) < 3 * LANES // 2, iota(tall, 0), iota(tall, 0) - 2 * LANES)
    lag_ref[...] = (source_at - iota(tall, 1)).astype(F32)
    idle = jnp.zeros((2 * LANES - 2 * MARGIN - reached, LANES), BF16)
    for p in range(slots):
        kernel_x[p, reached : 2 * LANES - 2 * MARGIN] = idle
    for load in loads[:2]:
        load.wait()
    tap_rows = jnp.broadcast_to(frac_ref[1:2].astype(F32), (8, slots))
    tap_rows = rounded(lanczos((REACH - iota((8, slots), 0)).astype(F32) - tap_rows))
    lag_rows = (iota((8, slots), 0) - REACH - jnp.broadcast_to(offset_ref[1:2], (8, slots))).astype(F32)
    for p in range(slots):
        tap_table[0, p] = jnp.broadcast_to(tap_rows[:, p : p + 1], (8, LANES))
        tap_table[1, p] = jnp.broadcast_to(lag_rows[:, p : p + 1], (8, LANES))
    ahead = ones_where(iota((rows, LANES), 1) < LANES // 2)
    behind = ones_where(iota((rows, LANES), 1) >= LANES // 2)

    def over_slots(step):
        lax.fori_loop(0, slots, lambda p, c: (step(p), c)[1], 0, unroll=slots <= 8)

    def build_kernel(p):
        for part_rows in (slice(0, reached), slice(2 * LANES - 2 * MARGIN, 2 * LANES)):
            lag = lag_ref[part_rows]
            total = jnp.zeros(lag.shape, F32)
            for t in range(TAPS):
                total = jnp.where(lag == tap_table[1, p, t : t + 1], tap_table[0, p, t : t + 1], total)
            kernel_x[p, part_rows] = total.astype(BF16)

    def warp_columns(b):
        def one_slot(p):
            count = cols // LANES
            source = [pixels[b, p, :, c * LANES : (c + 1) * LANES] for c in range(count)]
            blocks_in = []
            for c in range(count):
                beside = jnp.zeros((rows, LANES), BF16)
                if c + 1 < count:
                    beside = source[c + 1] * ahead
                if c:
                    beside = beside + source[c - 1] * behind
                blocks_in.append(jnp.concatenate([source[c], beside], 1))
            summed = dot(jnp.concatenate(blocks_in, 0), kernel_x[p]).astype(BF16)
            here = pl.ds(pl.multiple_of(p * rows, rows), rows)
            for c in range(count):
                e, first = c * LANES // part, c * LANES % part
                columns[e, b, here, first : first + LANES] = summed[c * rows : (c + 1) * rows]

        over_slots(one_slot)

    pixel_loads[0].wait()
    for load in loads[2:]:
        load.wait()
    over_slots(build_kernel)
    warp_columns(0)
    lane = iota((8, LANES), 1)
    small[...] = jnp.ones_like(small)
    tile = jnp.where(iota((1, slots), 1) < count_ref[0], tile_ref[...].astype(F32), NOBODY)
    small[TILE : TILE + 1] = jnp.full((1, LANES), NOBODY, F32)
    small[TILE : TILE + 1, :slots] = tile
    small[DY : DX + 1, :slots] = offset_ref[...].astype(F32)
    small[FY : FX + 1, :slots] = frac_ref[...].astype(F32)
    small[SIGMA:fields, :slots] = sigma_ref[...].astype(F32)
    by_lane = small[...]
    field_rows = by_lane.shape[0]
    place = ones_where(iota((16, LANES), 1) == iota((16, LANES), 0) + field_at)
    tall = jnp.concatenate([by_lane, jnp.zeros((16 - field_rows, LANES), F32)], 0) if field_rows < 16 else by_lane
    by_slot = dot_first(tall.astype(BF16), place[: tall.shape[0]])[:held_slots]
    cells = []
    for p in range(held_slots):
        if p < slots:
            cells.append(mask_ref[p].astype(F32))
            if blocks % 8:
                cells.append(jnp.zeros((-blocks % 8, mask_cols), F32))
        else:
            cells.append(jnp.zeros((blocks + -blocks % 8, mask_cols), F32))
    cells = jnp.concatenate(cells, 0)
    tall_blocks = blocks + -blocks % 8
    wide = (mask_cols, LANES)
    spread = ones_where((lax.rem(iota(wide, 1), mask_cols) == iota(wide, 0)) & (iota(wide, 1) < field_at))
    wide = dot(cells.astype(BF16), spread)
    wide = jnp.where(iota(wide.shape, 1) // mask_cols == lax.rem(iota(wide.shape, 0), tall_blocks), wide, 0.0)
    gather = (held_slots, held_slots * tall_blocks)
    by_slot = by_slot + dot(ones_where(iota(gather, 1) // tall_blocks == iota(gather, 0)), wide.astype(BF16))
    prior = jnp.concatenate([prior_ref[...], jnp.zeros((-bands % 8, rows), F32)], 0)
    prior = jnp.sum(prior, 1, keepdims=True)
    high = rounded(prior)
    middle = rounded(prior - high)
    by_lane = jnp.where(lane == PRIOR_LANE, high, by_lane)
    by_lane = jnp.where(lane == PRIOR_LANE + 1, middle, by_lane)
    by_lane = jnp.where(lane == PRIOR_LANE + 2, prior - high - middle, by_lane)
    group[0] = jnp.concatenate([by_slot, by_lane], 0).astype(BF16)

    def column(a, f):
        return a[:, field_at + f : field_at + f + 1]

    def slot_taps(a):
        at = iota(a.shape, 1)
        fraction = jnp.where(at < 8, column(a, FX), column(a, FY))
        return rounded(lanczos((REACH - lax.rem(at, 8)).astype(F32) - fraction))

    def column_cover(a, taps, first, width):
        at = (iota((a.shape[0], width), 1) + first).astype(F32) - column(a, DX)
        total = jnp.zeros(at.shape, F32)
        for t in range(TAPS):
            total = total + jnp.where(between(at + float(t - REACH), cols), taps[:, t : t + 1], 0.0)
        return jnp.clip(total, 0.0, 1.0)

    columns_copies, template_copies, group_copies, others_copies, flux_copies = {}, {}, {}, {}, {}
    pl.semaphore_wait(barrier, sky - 1 + epochs - 1)
    for d in range(1, epochs):
        group_copies[d] = remote(group.at[0], group.at[d], group_sem, (d - 1,), {"epoch": epoch_peer(d)})
    for b in range(bands):
        if b:
            pixel_loads[b].wait()
            warp_columns(b)
        for d in range(1, epochs):
            columns_copies[d, b] = remote(
                columns.at[epoch_peer(d), b], columns_held.at[d - 1, b], columns_sem, (d - 1, b),
                {"epoch": epoch_peer(d)},
            )
        for d in range(1, sky):
            template_copies[d, b] = remote(
                template_ref.at[b, :, own_cols], template_held.at[d - 1, b], template_sem, (d - 1, b),
                {"sky": sky_peer(d)},
            )
    flux[...] = jnp.zeros_like(flux)
    edge = jnp.zeros((bands, MARGIN, part), F32)
    framed[:, :MARGIN] = edge
    framed[:, MARGIN + sky * rows :] = edge
    own_rows = pl.ds(pl.multiple_of(MARGIN + me * rows, 8), rows)
    for b in range(bands):
        framed[b, own_rows] = template_ref[b, :, own_cols].astype(F32)

    depth_k = slots * rows
    cell_k = blocks * held_slots
    to_rows = ones_where(iota((LANES, depth_k), 1) // rows == iota((LANES, depth_k), 0))
    to_cells = (LANES, cell_k)
    to_cells = ones_where(
        (lax.rem(iota(to_cells, 1), held_slots) == iota(to_cells, 0)) & (iota(to_cells, 0) < slots)
    )

    def prepare(d, first_owner):
        message = group[d].astype(F32)
        a, by_lane = message[:held_slots], message[held_slots:]
        lanes = iota((held_slots, LANES), 1)
        same = (column(a, TILE) == by_lane[TILE : TILE + 1]) & (iota(lanes.shape, 0) < lanes)
        rank = jnp.sum(jnp.where(same, 1.0, 0.0), 0, keepdims=True)
        tap_rows = (REACH - iota((8, LANES), 0)).astype(F32) - by_lane[FY : FY + 1]
        tap_rows = rounded(lanczos(tap_rows))
        stack = jnp.concatenate(
            [tap_rows, jnp.broadcast_to(rank, (8, LANES)), by_lane] + [tap_rows] * (by_lane.shape[0] // 8 % 2), 0
        ).astype(BF16)
        k_stack = dot(stack, to_rows)
        gap = iota((canvas, depth_k), 0) - MARGIN - lax.rem(iota((canvas, depth_k), 1), rows)
        gap = gap.astype(F32) - k_stack[16 + DY : 17 + DY]
        row_table = jnp.zeros((canvas, depth_k), F32)
        for t in range(TAPS):
            row_table = row_table + jnp.where(gap == float(REACH - t), k_stack[t : t + 1], 0.0)
        c_stack = dot(stack, to_cells)
        c_lane = iota((canvas, cell_k), 1)
        reach = (iota((canvas, cell_k), 0) - MARGIN).astype(F32) - c_stack[16 + DY : 17 + DY]
        cover = jnp.zeros((canvas, cell_k), F32)
        for t in range(TAPS):
            cover = cover + jnp.where(between(reach + float(t - REACH), rows), c_stack[t : t + 1], 0.0)
        cover = jnp.clip(cover, 0.0, 1.0)
        cover = jnp.where(iota((canvas, cell_k), 0) // BLOCK_ROWS == c_lane // held_slots, cover, 0.0)
        cover = jnp.where(lax.rem(c_lane, held_slots) < slots, cover, 0.0)
        slot_cover = column_cover(a, slot_taps(a), epoch * part, part)
        chosen = [jnp.where(iota(a.shape, 1) // mask_cols == i, a, 0.0) for i in range(blocks)]
        wide = (LANES, part)
        spread = lax.rem(iota(wide, 0), mask_cols) == (iota(wide, 1) + epoch * part) // (cols // mask_cols)
        spread = ones_where(spread & (iota(wide, 0) < field_at))
        cells = dot(jnp.concatenate(chosen, 0).astype(BF16), spread)
        cells = (cells * jnp.concatenate([slot_cover] * blocks, 0)).astype(BF16)

        def here(stacked, owner, k):
            return (stacked[16 + TILE : 17 + TILE] == owner.astype(F32)) & (stacked[8:9] == float(k))

        pair_row = iota((pairs, LANES), 0)
        picked = (by_lane[TILE : TILE + 1] == (first_owner + pair_row // CAPACITY).astype(F32)) & (
            rank == lax.rem(pair_row, CAPACITY).astype(F32)
        ) & (iota((pairs, LANES), 1) < slots)
        for b in range(bands):
            scale = 1.0 / (CLIP_WIDTH * by_lane[SIGMA + b : SIGMA + b + 1])
            scale = jnp.sum(jnp.where(picked, scale, 0.0), 1, keepdims=True)
            inverse[d, b] = jnp.broadcast_to(scale, (pairs, LANES))
        sigma = [c_stack[16 + SIGMA + b : 17 + SIGMA + b] for b in range(bands)]
        weight = [cover * (CLIP_WIDTH / jnp.where(s > 0.0, s, 1.0)) for s in sigma]
        lhs = [[] for _ in range(bands)]
        for pair in range(pairs):
            owner, k = jnp.int32(first_owner + pair // CAPACITY), pair % CAPACITY
            at = slice(pair * canvas, (pair + 1) * canvas)
            left[d, at] = jnp.where(here(k_stack, owner, k), row_table, 0.0).astype(BF16)
            mine = here(c_stack, owner, k)
            for b in range(bands):
                lhs[b].append(jnp.where(mine, weight[b], 0.0))
        for b in range(bands):
            weigh[d, b] = dot(jnp.concatenate(lhs[b], 0).astype(BF16), cells)

    def process(d, b, first_owner):
        source = columns[epoch, b] if d == 0 else columns_held[d - 1, b]
        warped[...] = dot(left[d], source)
        for o in range(at_once):
            at = pl.ds(pl.multiple_of((first_owner + o) * rows, 8), canvas)
            frame = framed[b, at]
            total = flux[b, at]
            for k in range(CAPACITY):
                pair = o * CAPACITY + k
                here = slice(pair * canvas, (pair + 1) * canvas)
                scale = jnp.concatenate([inverse[d, b, pair : pair + 1]] * (part // LANES), 1)
                total = total + weigh[d, b, here] * jnp.tanh((warped[here] - frame) * scale)
            flux[b, at] = total

    def all_owners(step):
        if sky == at_once:
            step(0)
        else:
            lax.fori_loop(0, sky // at_once, lambda i, c: (step(i * at_once), c)[1], 0)

    for d in range(1, epochs):
        group_copies[d].wait_recv()
    for d in range(1, sky):
        others_copies[d] = remote(group, others.at[d - 1], others_sem, (d - 1,), {"sky": sky_peer(d)})
    if sky == at_once:
        for d in range(epochs):
            prepare(d, 0)
    for b in range(bands):
        for d in range(1, sky):
            template_copies[d, b].wait_recv()
            at = pl.ds(pl.multiple_of(MARGIN + lax.rem(me - d + sky, sky) * rows, 8), rows)
            framed[b, at] = template_held[d - 1, b].astype(F32)
        for d in range(epochs):
            if d:
                columns_copies[d, b].wait_recv()

            def step(first_owner, d=d, b=b):
                if sky != at_once:
                    prepare(d, first_owner)
                process(d, b, first_owner)

            all_owners(step)
        for d in range(1, sky):
            at = pl.ds(pl.multiple_of(MARGIN + sky_peer(d) * rows, 8), rows)
            send[d - 1, b] = flux[b, at].astype(BF16)
            flux_copies[d, b] = remote(
                send.at[d - 1, b], held.at[d - 1, b], flux_sem, (d - 1, b), {"sky": sky_peer(d)}
            )

    for d in range(1, sky):
        others_copies[d].wait_recv()
    square = (LANES, LANES)
    by_block = iota(square, 0) // BLOCK_ROWS == iota(square, 1) // mask_cols
    by_block = ones_where(by_block & (iota(square, 0) < canvas) & (iota(square, 1) < field_at))
    wide = (cols, LANES)
    by_cell = ones_where(iota(wide, 0) // (cols // mask_cols) == lax.rem(iota(wide, 1), mask_cols))
    wide = (LANES, part)
    to_cols = lax.rem(iota(wide, 0), mask_cols) == (iota(wide, 1) + epoch * part) // (cols // mask_cols)
    to_cols = ones_where(to_cols)

    def depth_from(groups):
        messages = [message[e] for message in groups for e in range(epochs)]
        every = jnp.concatenate([m[:held_slots].astype(F32) for m in messages], 0)
        prior_total = jnp.zeros((8, 1), F32)
        for message in messages[::epochs]:
            message = message[held_slots : held_slots + 8].astype(F32)
            prior_total = prior_total + jnp.sum(message[:, PRIOR_LANE : PRIOR_LANE + 3], 1, keepdims=True)
        number = every.shape[0]
        taps = slot_taps(every)
        cover = cover_ref.at[:number]
        cover[...] = column_cover(every, taps, 0, cols)
        at = iota((number, LANES), 1)

        def row_cover(row):
            total = jnp.zeros(row.shape, F32)
            for t in range(TAPS):
                total = total + jnp.where(between(row + float(t - REACH), rows), taps[:, 8 + t : 9 + t], 0.0)
            return jnp.clip(total, 0.0, 1.0)

        tile = column(every, TILE)
        row = (at - MARGIN).astype(F32)
        canvas_cover = row_cover(row - column(every, DY))
        in_patch = between(row + tile * float(rows), sky * rows) & (at < canvas)
        canvas_cover = jnp.where(in_patch, canvas_cover, 0.0)
        area = dot(canvas_cover.astype(BF16), by_block) * dot(cover[...].astype(BF16), by_cell)
        area = jnp.where(at < field_at, every * area, 0.0)
        area = jnp.sum(area, 1, keepdims=True)
        precision = [1.0 / (column(every, SIGMA + b) * column(every, SIGMA + b)) for b in range(bands)]
        totals = []
        for b in range(bands):
            total = jnp.sum(area * jnp.where(tile >= 0.0, precision[b], 0.0), 0, keepdims=True)
            totals.append(total + prior_total[b : b + 1] * float(cols))
        group_rows = rows // BLOCK_ROWS
        wide = (number, bands * rows)
        in_band = iota(wide, 1)
        row = (lax.rem(in_band, rows) + me * rows).astype(F32) - tile * float(rows) - column(every, DY)
        profile = row_cover(row)
        factor = jnp.zeros(wide, F32)
        for b in range(bands):
            factor = jnp.where(in_band // rows == b, precision[b], factor)
        profile = profile * factor
        block = lax.rem(in_band, rows) // BLOCK_ROWS
        lhs = jnp.concatenate([jnp.where(block == g, profile, 0.0) for g in range(group_rows)], 0).astype(BF16)
        first = MARGIN // BLOCK_ROWS
        canvas_block = (first + group_rows * me).astype(F32) - tile * float(group_rows)
        chosen = [
            jnp.where(((at // mask_cols).astype(F32) == canvas_block + float(g)) & (at < field_at), every, 0.0)
            for g in range(group_rows)
        ]
        cells = dot(jnp.concatenate(chosen, 0).astype(BF16), to_cols)
        own_cover = cover[:, own_cols]
        cells = (cells * jnp.concatenate([own_cover] * group_rows, 0)).astype(BF16)
        return (dot_first(lhs, cells), *totals)

    if sky <= AT_ONCE:
        weights, *totals = depth_from([group[...]] + [others[d - 1] for d in range(1, sky)])
    else:
        weights, *totals = lax.fori_loop(
            0, sky - 1,
            lambda d, sums: tuple(x + y for x, y in zip(sums, depth_from([others[d]]))),
            depth_from([group[...]]),
        )
    means = [total * (1.0 / (sky * rows * cols)) for total in totals]
    diagonal = iota((rows, rows), 0) == iota((rows, rows), 1)
    depths = []
    for b in range(bands):
        prior = jnp.sum(jnp.where(diagonal, prior_ref[b : b + 1], 0.0), 1, keepdims=True)
        depth = weights[b * rows : (b + 1) * rows] + prior
        depth_ref[b] = (depth / means[b]).astype(BF16)
        depths.append(depth)
    for b in range(bands):
        total = flux[b, own_rows]
        for d in range(1, sky):
            flux_copies[d, b].wait_recv()
            total = total + held[d - 1, b].astype(F32)
        coadd_ref[b] = (framed[b, own_rows] + total / depths[b]).astype(BF16)
    for copies in (group_copies, others_copies, template_copies, columns_copies, flux_copies):
        for copy in copies.values():
            copy.wait_send()


def leave_kernel(coadd_in, depth_in, coadd_ref, depth_ref, sem):
    copies = [
        pltpu.make_async_copy(coadd_in, coadd_ref, sem.at[0]),
        pltpu.make_async_copy(depth_in, depth_ref, sem.at[1]),
    ]
    for copy in copies:
        copy.start()
    for copy in copies:
        copy.wait()


def on_device(
    slot_pixels, slot_tile, slot_offset, slot_frac, slot_sigma, clip_mask, slot_count, template, prior_weight
):
    sky = lax.axis_size("sky")
    epochs = lax.axis_size("epoch")
    slots, bands, rows, cols = slot_pixels.shape
    blocks, mask_cols = clip_mask.shape[1:]
    part = cols // epochs
    canvas = rows + 2 * MARGIN
    held_slots = slots + -slots % 8
    field_rows = SIGMA + bands + -(SIGMA + bands) % 8
    message = held_slots + field_rows
    at_once = sky if sky <= AT_ONCE else 1
    pairs = at_once * CAPACITY
    vmem = pl.BlockSpec(memory_space=pltpu.VMEM)
    block = jax.ShapeDtypeStruct((bands, rows, part), BF16)
    patch = sky * rows + 2 * MARGIN
    limit = 32 * 1024 * 1024 if sky <= AT_ONCE else None
    results = pl.pallas_call(
        functools.partial(coadd_kernel, (bands, sky, epochs, rows, cols, slots, blocks, mask_cols)),
        out_shape=(block, block),
        in_specs=[pl.BlockSpec(memory_space=pltpu.SMEM)] + [pl.BlockSpec(memory_space=pltpu.MemorySpace.HBM)] * 8,
        out_specs=(vmem, vmem),
        scratch_shapes=[
            pltpu.VMEM((2, slots), jnp.int32),
            pltpu.VMEM((2, slots), BF16),
            pltpu.VMEM((bands, rows, cols), BF16),
            pltpu.VMEM((1, slots), jnp.int32),
            pltpu.VMEM((bands, slots), BF16),
            pltpu.VMEM((slots, blocks, mask_cols), jnp.int32),
            pltpu.VMEM((bands, rows), F32),
            pltpu.VMEM((bands, slots, rows, cols), BF16),
            pltpu.VMEM((field_rows, LANES), F32),
            pltpu.VMEM((epochs, message, LANES), BF16),
            pltpu.VMEM((sky - 1, epochs, message, LANES), BF16),
            pltpu.VMEM((2, slots, 8, LANES), F32),
            pltpu.VMEM((2 * LANES, LANES), F32),
            pltpu.VMEM((slots, 2 * LANES, LANES), BF16),
            pltpu.VMEM((epochs, bands, slots * rows, part), BF16),
            pltpu.VMEM((epochs - 1, bands, slots * rows, part), BF16),
            pltpu.VMEM((sky - 1, bands, rows, part), BF16),
            pltpu.VMEM((bands, patch, part), F32),
            pltpu.VMEM((bands, patch, part), F32),
            pltpu.VMEM((epochs, pairs * canvas, slots * rows), BF16),
            pltpu.VMEM((epochs, bands, pairs * canvas, part), F32),
            pltpu.VMEM((epochs, bands, pairs, LANES), F32),
            pltpu.VMEM((pairs * canvas, part), F32),
            pltpu.VMEM((sky - 1, bands, rows, part), BF16),
            pltpu.VMEM((sky - 1, bands, rows, part), BF16),
            pltpu.VMEM(((sky if sky <= AT_ONCE else 1) * epochs * held_slots, cols), F32),
            pltpu.SemaphoreType.DMA((bands + 7,)),
            pltpu.SemaphoreType.DMA((2, epochs - 1)),
            pltpu.SemaphoreType.DMA((2, sky - 1)),
            pltpu.SemaphoreType.DMA((2, sky - 1, bands)),
            pltpu.SemaphoreType.DMA((2, epochs - 1, bands)),
            pltpu.SemaphoreType.DMA((2, sky - 1, bands)),
        ],
        compiler_params=pltpu.CompilerParams(collective_id=0, has_side_effects=True, vmem_limit_bytes=limit),
        name="coadd",
    )(*[
        x if x is slot_count else pltpu.with_memory_space_constraint(x, pltpu.MemorySpace.HBM)
        for x in (
            slot_count, slot_offset.T, slot_frac.T, slot_pixels, template, slot_tile.T, slot_sigma.T,
            clip_mask, prior_weight,
        )
    ])

    return pl.pallas_call(
        leave_kernel,
        out_shape=(block, block),
        in_specs=[vmem] * 2,
        out_specs=(pl.BlockSpec(memory_space=pl.ANY),) * 2,
        scratch_shapes=[pltpu.SemaphoreType.DMA((2,))],
        compiler_params=pltpu.CompilerParams(vmem_limit_bytes=1024 * 1024),
        name="leave",
    )(*results)


def solution(mesh):
    in_specs = (
        P(("groups", "sky", "epoch"), "band", None, None),
        P(("groups", "sky", "epoch"), None),
        P(("groups", "sky", "epoch"), None),
        P(("groups", "sky", "epoch"), None),
        P(("groups", "sky", "epoch"), "band"),
        P(("groups", "sky", "epoch"), None, None),
        P(("groups", "sky", "epoch")),
        P("band", ("groups", "sky"), None),
        P("band", ("groups", "sky")),
    )
    out_specs = (P("band", ("groups", "sky"), "epoch"), P("band", ("groups", "sky"), "epoch"))
    return jax.shard_map(
        on_device, mesh=mesh, in_specs=in_specs, out_specs=out_specs, check_vma=False
    )
```

```python
import functools
import math

import jax
import jax.numpy as jnp
from jax import lax
from jax.experimental import pallas as pl
from jax.experimental.pallas import tpu as pltpu
from jax.sharding import PartitionSpec as P

MARGIN = 8
BLOCK_ROWS = 8
REACH = 3
TAPS = 2 * REACH
LANES = 128
CAPACITY = 2
CLIP_WIDTH = 3.0
NOBODY = -64.0
PRIOR_LANE = 64
AT_ONCE = 4
TILE, DY, DX, FY, FX, SIGMA = range(6)
MESH = pl.DeviceIdType.MESH
F32 = jnp.float32
BF16 = jnp.bfloat16

def sinc(x):
    at_zero = x == 0.0
    turned = math.pi * jnp.where(at_zero, 1.0, x)
    return jnp.where(at_zero, 1.0, jnp.sin(turned) / turned)

def lanczos(distance):
    inside = jnp.abs(distance) < 3.0
    return jnp.where(inside, sinc(distance) * sinc(distance / 3.0), 0.0)

def rounded(x):
    return x.astype(BF16).astype(F32)

def iota(shape, dim):
    return lax.broadcasted_iota(jnp.int32, shape, dim)

def ones_where(condition):
    return jnp.where(condition, 1.0, 0.0).astype(BF16)

def dot(a, b):
    return jnp.dot(a, b, preferred_element_type=F32)

def dot_first(a, b):
    return lax.dot_general(a, b, (((0,), (0,)), ((), ())), preferred_element_type=F32)

def between(x, extent):
    return (x >= 0.0) & (x < float(extent))

def coadd_kernel(
    shape, *refs,
):
    count_ref, *inputs = refs[:9]
    (
        coadd_ref, depth_ref,
        offset_ref, frac_ref, template_ref, tile_ref, sigma_ref, mask_ref, prior_ref,
        pixels, small, group, others, tap_table, lag_ref, kernel_x, columns, columns_held, template_held,
        framed, flux, left, weigh, inverse, send, held, cover_ref,
        local_sem, message_sem, template_sem, columns_sem, flux_sem, sent_sem,
    ) = refs[9:]
    bands, sky, epochs, rows, cols, slots, blocks, mask_cols = shape
    part = cols // epochs
    canvas = rows + 2 * MARGIN
    padded = cols + LANES
    held_slots = slots + -slots % 8
    fields = SIGMA + bands
    field_at = blocks * mask_cols
    at_once = sky if sky <= AT_ONCE else 1
    pairs = at_once * CAPACITY
    me = lax.axis_index("sky")
    epoch = lax.axis_index("epoch")
    own_cols = pl.ds(pl.multiple_of(epoch * part, LANES), part)

    def sky_peer(d):
        return lax.rem(me + d, sky)

    def epoch_peer(d):
        return lax.rem(epoch + d, epochs)

    barrier = pltpu.get_barrier_semaphore()
    for d in range(1, sky):
        pl.semaphore_signal(barrier, inc=1, device_id={"sky": sky_peer(d)}, device_id_type=MESH)
    for d in range(1, epochs):
        pl.semaphore_signal(barrier, inc=1, device_id={"epoch": epoch_peer(d)}, device_id_type=MESH)
    targets = [offset_ref, frac_ref, pixels.at[0], template_ref, tile_ref, sigma_ref, mask_ref, prior_ref]
    targets += [pixels.at[b] for b in range(1, bands)]
    sources = inputs[:2] + [inputs[2].at[:, 0]] + inputs[3:] + [inputs[2].at[:, b] for b in range(1, bands)]
    loads = []
    for i, (source, target) in enumerate(zip(sources, targets)):
        loads.append(pltpu.make_async_copy(source, target, local_sem.at[i]))
        loads[-1].start()

    def remote(src, dst, sent, received, where):
        pltpu.make_async_remote_copy(
            src_ref=src, dst_ref=dst, send_sem=sent, recv_sem=received, device_id=where, device_id_type=MESH
        ).start()

    def wait_bytes(ref, sem):
        pltpu.make_async_copy(ref, ref, sem).wait()

    halves = 2 if part % (2 * LANES) == 0 else 1
    chunks = []
    for b in range(bands):
        pieces = halves if b in (0, bands - 1) else 1
        chunks += [(b, i * (part // pieces), part // pieces) for i in range(pieces)]

    tall = (2 * LANES, LANES)
    reached = LANES + 2 * MARGIN
    source_at = jnp.where(iota(tall, 0) < 3 * LANES // 2, iota(tall, 0), iota(tall, 0) - 2 * LANES)
    lag_ref[...] = (source_at - iota(tall, 1)).astype(F32)
    idle = jnp.zeros((2 * LANES - 2 * MARGIN - reached, LANES), BF16)
    for p in range(slots):
        kernel_x[p, reached : 2 * LANES - 2 * MARGIN] = idle
    for load in loads[:2]:
        load.wait()
    tap_rows = jnp.broadcast_to(frac_ref[1:2].astype(F32), (8, slots))
    tap_rows = rounded(lanczos((REACH - iota((8, slots), 0)).astype(F32) - tap_rows))
    lag_rows = (iota((8, slots), 0) - REACH - jnp.broadcast_to(offset_ref[1:2], (8, slots))).astype(F32)
    for p in range(slots):
        tap_table[0, p] = jnp.broadcast_to(tap_rows[:, p : p + 1], (8, LANES))
        tap_table[1, p] = jnp.broadcast_to(lag_rows[:, p : p + 1], (8, LANES))
    ahead = ones_where(iota((rows, LANES), 1) < LANES // 2)
    behind = ones_where(iota((rows, LANES), 1) >= LANES // 2)

    def over_slots(step):
        lax.fori_loop(0, slots, lambda p, c: (step(p), c)[1], 0, unroll=slots <= 8)

    def build_kernel(p):
        for part_rows in (slice(0, reached), slice(2 * LANES - 2 * MARGIN, 2 * LANES)):
            lag = lag_ref[part_rows]
            total = jnp.zeros(lag.shape, F32)
            for t in range(TAPS):
                total = jnp.where(lag == tap_table[1, p, t : t + 1], tap_table[0, p, t : t + 1], total)
            kernel_x[p, part_rows] = total.astype(BF16)

    def warp_columns(b):
        def one_slot(p):
            count = cols // LANES
            source = [pixels[b, p, :, c * LANES : (c + 1) * LANES] for c in range(count)]
            blocks_in = []
            for c in range(count):
                beside = jnp.zeros((rows, LANES), BF16)
                if c + 1 < count:
                    beside = source[c + 1] * ahead
                if c:
                    beside = beside + source[c - 1] * behind
                blocks_in.append(jnp.concatenate([source[c], beside], 1))
            summed = dot(jnp.concatenate(blocks_in, 0), kernel_x[p]).astype(BF16)
            here = pl.ds(pl.multiple_of(p * rows, rows), rows)
            for c in range(count):
                e, first = c * LANES // part, c * LANES % part
                columns[e, b, here, first : first + LANES] = summed[c * rows : (c + 1) * rows]

        over_slots(one_slot)

    near_core = lax.axis_index("band") > 0

    def send_columns(i):
        if chunks[i][0] == 0:
            send_columns_now(i)
        else:
            pl.when(jnp.logical_not(near_core))(functools.partial(send_columns_now, i))

    def send_columns_now(i):
        b, first, width = chunks[i]
        at = pl.ds(first, width)
        for d in range(1, epochs):
            remote(
                columns.at[epoch_peer(d), b, :, at], columns_held.at[d - 1, b, :, at],
                sent_sem.at[0], columns_sem.at[i], {"epoch": epoch_peer(d)},
            )

    def send_template(b):
        for d in range(1, sky):
            remote(
                template_ref.at[b, :, own_cols], template_held.at[d - 1, b],
                sent_sem.at[1], template_sem.at[b], {"sky": sky_peer(d)},
            )

    for load in loads[2:8]:
        load.wait()

    over_slots(build_kernel)
    warp_columns(0)
    lane = iota((8, LANES), 1)
    small[...] = jnp.ones_like(small)
    tile = jnp.where(iota((1, slots), 1) < count_ref[0], tile_ref[...].astype(F32), NOBODY)
    small[TILE : TILE + 1] = jnp.full((1, LANES), NOBODY, F32)
    small[TILE : TILE + 1, :slots] = tile
    small[DY : DX + 1, :slots] = offset_ref[...].astype(F32)
    small[FY : FX + 1, :slots] = frac_ref[...].astype(F32)
    small[SIGMA:fields, :slots] = sigma_ref[...].astype(F32)
    by_lane = small[...]
    field_rows = by_lane.shape[0]
    place = ones_where(iota((16, LANES), 1) == iota((16, LANES), 0) + field_at)
    tall = jnp.concatenate([by_lane, jnp.zeros((16 - field_rows, LANES), F32)], 0) if field_rows < 16 else by_lane
    by_slot = dot_first(tall.astype(BF16), place[: tall.shape[0]])[:held_slots]
    cells = []
    for p in range(held_slots):
        if p < slots:
            cells.append(mask_ref[p].astype(F32))
            if blocks % 8:
                cells.append(jnp.zeros((-blocks % 8, mask_cols), F32))
        else:
            cells.append(jnp.zeros((blocks + -blocks % 8, mask_cols), F32))
    cells = jnp.concatenate(cells, 0)
    tall_blocks = blocks + -blocks % 8
    wide = (mask_cols, LANES)
    spread = ones_where((lax.rem(iota(wide, 1), mask_cols) == iota(wide, 0)) & (iota(wide, 1) < field_at))
    wide = dot(cells.astype(BF16), spread)
    wide = jnp.where(iota(wide.shape, 1) // mask_cols == lax.rem(iota(wide.shape, 0), tall_blocks), wide, 0.0)
    gather = (held_slots, held_slots * tall_blocks)
    by_slot = by_slot + dot(ones_where(iota(gather, 1) // tall_blocks == iota(gather, 0)), wide.astype(BF16))
    prior = jnp.concatenate([prior_ref[...], jnp.zeros((-bands % 8, rows), F32)], 0)
    prior = jnp.sum(prior, 1, keepdims=True)
    high = rounded(prior)
    middle = rounded(prior - high)
    by_lane = jnp.where(lane == PRIOR_LANE, high, by_lane)
    by_lane = jnp.where(lane == PRIOR_LANE + 1, middle, by_lane)
    by_lane = jnp.where(lane == PRIOR_LANE + 2, prior - high - middle, by_lane)
    group[0] = jnp.concatenate([by_slot, by_lane], 0).astype(BF16)

    def column(a, f):
        return a[:, field_at + f : field_at + f + 1]

    def slot_taps(a):
        at = iota(a.shape, 1)
        fraction = jnp.where(at < 8, column(a, FX), column(a, FY))
        return rounded(lanczos((REACH - lax.rem(at, 8)).astype(F32) - fraction))

    def column_cover(a, taps, first, width):
        at = (iota((a.shape[0], width), 1) + first).astype(F32) - column(a, DX)
        total = jnp.zeros(at.shape, F32)
        for t in range(TAPS):
            total = total + jnp.where(between(at + float(t - REACH), cols), taps[:, t : t + 1], 0.0)
        return jnp.clip(total, 0.0, 1.0)

    pl.semaphore_wait(barrier, sky - 1 + epochs - 1)

    for d in range(1, epochs):
        remote(group.at[0], group.at[d], sent_sem.at[2], message_sem.at[0], {"epoch": epoch_peer(d)})
    for i in range(halves):
        send_columns(i)
    send_template(0)
    for b in range(1, bands):

        loads[7 + b].wait()
        warp_columns(b)

        for i, chunk in enumerate(chunks):
            if chunk[0] == b:
                send_columns(i)
        send_template(b)

    flux[...] = jnp.zeros_like(flux)
    edge = jnp.zeros((bands, MARGIN, part), F32)
    framed[:, :MARGIN] = edge
    framed[:, MARGIN + sky * rows :] = edge
    own_rows = pl.ds(pl.multiple_of(MARGIN + me * rows, 8), rows)
    for b in range(bands):
        framed[b, own_rows] = template_ref[b, :, own_cols].astype(F32)

    depth_k = slots * rows
    cell_k = blocks * held_slots
    to_rows = ones_where(iota((LANES, depth_k), 1) // rows == iota((LANES, depth_k), 0))
    to_cells = (LANES, cell_k)
    to_cells = ones_where(
        (lax.rem(iota(to_cells, 1), held_slots) == iota(to_cells, 0)) & (iota(to_cells, 0) < slots)
    )

    def prepare(d, first_owner):
        message = group[d].astype(F32)
        a, by_lane = message[:held_slots], message[held_slots:]
        lanes = iota((held_slots, LANES), 1)
        same = (column(a, TILE) == by_lane[TILE : TILE + 1]) & (iota(lanes.shape, 0) < lanes)
        rank = jnp.sum(jnp.where(same, 1.0, 0.0), 0, keepdims=True)
        tap_rows = (REACH - iota((8, LANES), 0)).astype(F32) - by_lane[FY : FY + 1]
        tap_rows = rounded(lanczos(tap_rows))
        stack = jnp.concatenate(
            [tap_rows, jnp.broadcast_to(rank, (8, LANES)), by_lane] + [tap_rows] * (by_lane.shape[0] // 8 % 2), 0
        ).astype(BF16)
        k_stack = dot(stack, to_rows)
        gap = iota((canvas, depth_k), 0) - MARGIN - lax.rem(iota((canvas, depth_k), 1), rows)
        gap = gap.astype(F32) - k_stack[16 + DY : 17 + DY]
        row_table = jnp.zeros((canvas, depth_k), F32)
        for t in range(TAPS):
            row_table = row_table + jnp.where(gap == float(REACH - t), k_stack[t : t + 1], 0.0)
        c_stack = dot(stack, to_cells)
        c_lane = iota((canvas, cell_k), 1)
        reach = (iota((canvas, cell_k), 0) - MARGIN).astype(F32) - c_stack[16 + DY : 17 + DY]
        cover = jnp.zeros((canvas, cell_k), F32)
        for t in range(TAPS):
            cover = cover + jnp.where(between(reach + float(t - REACH), rows), c_stack[t : t + 1], 0.0)
        cover = jnp.clip(cover, 0.0, 1.0)
        cover = jnp.where(iota((canvas, cell_k), 0) // BLOCK_ROWS == c_lane // held_slots, cover, 0.0)
        cover = jnp.where(lax.rem(c_lane, held_slots) < slots, cover, 0.0)
        slot_cover = column_cover(a, slot_taps(a), epoch * part, part)
        chosen = [jnp.where(iota(a.shape, 1) // mask_cols == i, a, 0.0) for i in range(blocks)]
        wide = (LANES, part)
        spread = lax.rem(iota(wide, 0), mask_cols) == (iota(wide, 1) + epoch * part) // (cols // mask_cols)
        spread = ones_where(spread & (iota(wide, 0) < field_at))
        cells = dot(jnp.concatenate(chosen, 0).astype(BF16), spread)
        cells = (cells * jnp.concatenate([slot_cover] * blocks, 0)).astype(BF16)

        def here(stacked, owner, k):
            return (stacked[16 + TILE : 17 + TILE] == owner.astype(F32)) & (stacked[8:9] == float(k))

        pair_row = iota((pairs, LANES), 0)
        picked = (by_lane[TILE : TILE + 1] == (first_owner + pair_row // CAPACITY).astype(F32)) & (
            rank == lax.rem(pair_row, CAPACITY).astype(F32)
        ) & (iota((pairs, LANES), 1) < slots)
        for b in range(bands):
            scale = 1.0 / (CLIP_WIDTH * by_lane[SIGMA + b : SIGMA + b + 1])
            scale = jnp.sum(jnp.where(picked, scale, 0.0), 1, keepdims=True)
            inverse[d, b] = jnp.broadcast_to(scale, (pairs, LANES))
        sigma = [c_stack[16 + SIGMA + b : 17 + SIGMA + b] for b in range(bands)]
        weight = [cover * (CLIP_WIDTH / jnp.where(s > 0.0, s, 1.0)) for s in sigma]
        lhs = [[] for _ in range(bands)]
        for pair in range(pairs):
            owner, k = jnp.int32(first_owner + pair // CAPACITY), pair % CAPACITY
            at = slice(pair * canvas, (pair + 1) * canvas)
            left[d, at] = jnp.where(here(k_stack, owner, k), row_table, 0.0).astype(BF16)
            mine = here(c_stack, owner, k)
            for b in range(bands):
                lhs[b].append(jnp.where(mine, weight[b], 0.0))
        for b in range(bands):
            weigh[d, b] = dot(jnp.concatenate(lhs[b], 0).astype(BF16), cells)

    def process(d, chunk, first_owner):
        b, first, width = chunk
        lanes = slice(first, first + width)
        source = columns[epoch, b, :, lanes] if d == 0 else columns_held[d - 1, b, :, lanes]
        for o in range(at_once):
            at = pl.ds(pl.multiple_of((first_owner + o) * rows, 8), canvas)
            frame = framed[b, at, lanes]
            total = flux[b, at, lanes]
            both = slice(o * CAPACITY * canvas, (o + 1) * CAPACITY * canvas)
            warped = dot(left[d, both], source)
            for k in range(CAPACITY):
                pair = o * CAPACITY + k
                here = slice(pair * canvas, (pair + 1) * canvas)
                scale = jnp.concatenate([inverse[d, b, pair : pair + 1]] * (width // LANES), 1)
                total = total + weigh[d, b, here, lanes] * jnp.tanh((warped[k * canvas : (k + 1) * canvas] - frame) * scale)
            flux[b, at, lanes] = total

    def all_owners(step):
        if sky == at_once:
            step(0)
        else:
            lax.fori_loop(0, sky // at_once, lambda i, c: (step(i * at_once), c)[1], 0)

    if sky == at_once:
        prepare(0, 0)

    def send_held_back():
        for i, chunk in enumerate(chunks):
            if chunk[0] > 0:
                send_columns_now(i)

    def meet_epoch_peers():
        wait_bytes(group.at[1:], message_sem.at[0])
        for d in range(1, sky):
            remote(group, others.at[d - 1], sent_sem.at[3], message_sem.at[1], {"sky": sky_peer(d)})
        if sky == at_once:

            for d in range(1, epochs):
                prepare(d, 0)

    meet_epoch_peers()
    for i, chunk in enumerate(chunks):
        b, first, width = chunk
        lanes = slice(first, first + width)
        if first == 0:

            wait_bytes(template_held.at[:, b], template_sem.at[b])
            for d in range(1, sky):
                at = pl.ds(pl.multiple_of(MARGIN + lax.rem(me - d + sky, sky) * rows, 8), rows)
                framed[b, at] = template_held[d - 1, b].astype(F32)
        if i == 0:
            pl.when(near_core)(send_held_back)
        for d in range(epochs):
            if d == 1:

                wait_bytes(columns_held.at[:, b, :, pl.ds(first, width)], columns_sem.at[i])

            def step(first_owner, d=d, chunk=chunk):
                if sky != at_once:
                    prepare(d, first_owner)
                process(d, chunk, first_owner)

            all_owners(step)

        for d in range(1, sky):
            at = pl.ds(pl.multiple_of(MARGIN + sky_peer(d) * rows, 8), rows)
            send[d - 1, b, :, lanes] = flux[b, at, lanes].astype(BF16)
        for d in range(1, sky):
            at = pl.ds(first, width)
            remote(
                send.at[d - 1, b, :, at], held.at[d - 1, b, :, at],
                sent_sem.at[4], flux_sem.at[i], {"sky": sky_peer(d)},
            )


    wait_bytes(others, message_sem.at[1])

    square = (LANES, LANES)
    by_block = iota(square, 0) // BLOCK_ROWS == iota(square, 1) // mask_cols
    by_block = ones_where(by_block & (iota(square, 0) < canvas) & (iota(square, 1) < field_at))
    wide = (cols, LANES)
    by_cell = ones_where(iota(wide, 0) // (cols // mask_cols) == lax.rem(iota(wide, 1), mask_cols))
    wide = (LANES, part)
    to_cols = lax.rem(iota(wide, 0), mask_cols) == (iota(wide, 1) + epoch * part) // (cols // mask_cols)
    to_cols = ones_where(to_cols)

    def depth_from(groups):
        messages = [message[e] for message in groups for e in range(epochs)]
        every = jnp.concatenate([m[:held_slots].astype(F32) for m in messages], 0)
        prior_total = jnp.zeros((8, 1), F32)
        for message in messages[::epochs]:
            message = message[held_slots : held_slots + 8].astype(F32)
            prior_total = prior_total + jnp.sum(message[:, PRIOR_LANE : PRIOR_LANE + 3], 1, keepdims=True)
        number = every.shape[0]
        taps = slot_taps(every)
        cover = cover_ref.at[:number]
        cover[...] = column_cover(every, taps, 0, cols)
        at = iota((number, LANES), 1)

        def row_cover(row):
            total = jnp.zeros(row.shape, F32)
            for t in range(TAPS):
                total = total + jnp.where(between(row + float(t - REACH), rows), taps[:, 8 + t : 9 + t], 0.0)
            return jnp.clip(total, 0.0, 1.0)

        tile = column(every, TILE)
        row = (at - MARGIN).astype(F32)
        canvas_cover = row_cover(row - column(every, DY))
        in_patch = between(row + tile * float(rows), sky * rows) & (at < canvas)
        canvas_cover = jnp.where(in_patch, canvas_cover, 0.0)
        area = dot(canvas_cover.astype(BF16), by_block) * dot(cover[...].astype(BF16), by_cell)
        area = jnp.where(at < field_at, every * area, 0.0)
        area = jnp.sum(area, 1, keepdims=True)
        precision = [1.0 / (column(every, SIGMA + b) * column(every, SIGMA + b)) for b in range(bands)]
        totals = []
        for b in range(bands):
            total = jnp.sum(area * jnp.where(tile >= 0.0, precision[b], 0.0), 0, keepdims=True)
            totals.append(total + prior_total[b : b + 1] * float(cols))
        group_rows = rows // BLOCK_ROWS
        wide = (number, bands * rows)
        in_band = iota(wide, 1)
        row = (lax.rem(in_band, rows) + me * rows).astype(F32) - tile * float(rows) - column(every, DY)
        profile = row_cover(row)
        factor = jnp.zeros(wide, F32)
        for b in range(bands):
            factor = jnp.where(in_band // rows == b, precision[b], factor)
        profile = profile * factor
        block = lax.rem(in_band, rows) // BLOCK_ROWS
        lhs = jnp.concatenate([jnp.where(block == g, profile, 0.0) for g in range(group_rows)], 0).astype(BF16)
        first = MARGIN // BLOCK_ROWS
        canvas_block = (first + group_rows * me).astype(F32) - tile * float(group_rows)
        chosen = [
            jnp.where(((at // mask_cols).astype(F32) == canvas_block + float(g)) & (at < field_at), every, 0.0)
            for g in range(group_rows)
        ]
        cells = dot(jnp.concatenate(chosen, 0).astype(BF16), to_cols)
        own_cover = cover[:, own_cols]
        cells = (cells * jnp.concatenate([own_cover] * group_rows, 0)).astype(BF16)
        return (dot_first(lhs, cells), *totals)

    if sky <= AT_ONCE:
        weights, *totals = depth_from([group[...]] + [others[d - 1] for d in range(1, sky)])
    else:
        weights, *totals = lax.fori_loop(
            0, sky - 1,
            lambda d, sums: tuple(x + y for x, y in zip(sums, depth_from([others[d]]))),
            depth_from([group[...]]),
        )
    means = [total * (1.0 / (sky * rows * cols)) for total in totals]
    diagonal = iota((rows, rows), 0) == iota((rows, rows), 1)
    depths = []
    for b in range(bands):
        prior = jnp.sum(jnp.where(diagonal, prior_ref[b : b + 1], 0.0), 1, keepdims=True)
        depth = weights[b * rows : (b + 1) * rows] + prior
        depth_ref[b] = (depth / means[b]).astype(BF16)
        depths.append(depth)

    for sent, ref in enumerate((columns_held, template_held, group.at[1:], others)):
        wait_bytes(ref, sent_sem.at[sent])
    for i, (b, first, width) in enumerate(chunks):
        lanes = slice(first, first + width)

        wait_bytes(held.at[:, b, :, pl.ds(first, width)], flux_sem.at[i])

        total = flux[b, own_rows, lanes]
        for d in range(1, sky):
            total = total + held[d - 1, b, :, lanes].astype(F32)
        coadd_ref[b, :, lanes] = (framed[b, own_rows, lanes] + total / depths[b][:, lanes]).astype(BF16)

    wait_bytes(send, sent_sem.at[4])

def leave_kernel(coadd_in, depth_in, coadd_ref, depth_ref, sem):
    copies = [
        pltpu.make_async_copy(coadd_in, coadd_ref, sem.at[0]),
        pltpu.make_async_copy(depth_in, depth_ref, sem.at[1]),
    ]
    for copy in copies:
        copy.start()
    for copy in copies:
        copy.wait()

def on_device(
    slot_pixels, slot_tile, slot_offset, slot_frac, slot_sigma, clip_mask, slot_count, template, prior_weight
):
    sky = lax.axis_size("sky")
    epochs = lax.axis_size("epoch")
    slots, bands, rows, cols = slot_pixels.shape
    blocks, mask_cols = clip_mask.shape[1:]
    part = cols // epochs
    canvas = rows + 2 * MARGIN
    held_slots = slots + -slots % 8
    field_rows = SIGMA + bands + -(SIGMA + bands) % 8
    message = held_slots + field_rows
    at_once = sky if sky <= AT_ONCE else 1
    pairs = at_once * CAPACITY
    vmem = pl.BlockSpec(memory_space=pltpu.VMEM)
    block = jax.ShapeDtypeStruct((bands, rows, part), BF16)
    patch = sky * rows + 2 * MARGIN
    limit = 32 * 1024 * 1024 if sky <= AT_ONCE else None
    results = pl.pallas_call(
        functools.partial(coadd_kernel, (bands, sky, epochs, rows, cols, slots, blocks, mask_cols)),
        out_shape=(block, block),
        in_specs=[pl.BlockSpec(memory_space=pltpu.SMEM)] + [pl.BlockSpec(memory_space=pltpu.MemorySpace.HBM)] * 8,
        out_specs=(vmem, vmem),
        scratch_shapes=[
            pltpu.VMEM((2, slots), jnp.int32),
            pltpu.VMEM((2, slots), BF16),
            pltpu.VMEM((bands, rows, cols), BF16),
            pltpu.VMEM((1, slots), jnp.int32),
            pltpu.VMEM((bands, slots), BF16),
            pltpu.VMEM((slots, blocks, mask_cols), jnp.int32),
            pltpu.VMEM((bands, rows), F32),
            pltpu.VMEM((bands, slots, rows, cols), BF16),
            pltpu.VMEM((field_rows, LANES), F32),
            pltpu.VMEM((epochs, message, LANES), BF16),
            pltpu.VMEM((sky - 1, epochs, message, LANES), BF16),
            pltpu.VMEM((2, slots, 8, LANES), F32),
            pltpu.VMEM((2 * LANES, LANES), F32),
            pltpu.VMEM((slots, 2 * LANES, LANES), BF16),
            pltpu.VMEM((epochs, bands, slots * rows, part), BF16),
            pltpu.VMEM((epochs - 1, bands, slots * rows, part), BF16),
            pltpu.VMEM((sky - 1, bands, rows, part), BF16),
            pltpu.VMEM((bands, patch, part), F32),
            pltpu.VMEM((bands, patch, part), F32),
            pltpu.VMEM((epochs, pairs * canvas, slots * rows), BF16),
            pltpu.VMEM((epochs, bands, pairs * canvas, part), F32),
            pltpu.VMEM((epochs, bands, pairs, LANES), F32),
            pltpu.VMEM((sky - 1, bands, rows, part), BF16),
            pltpu.VMEM((sky - 1, bands, rows, part), BF16),
            pltpu.VMEM(((sky if sky <= AT_ONCE else 1) * epochs * held_slots, cols), F32),
            pltpu.SemaphoreType.DMA((bands + 7,)),
            pltpu.SemaphoreType.DMA((2,)),
            pltpu.SemaphoreType.DMA((bands,)),
            pltpu.SemaphoreType.DMA((bands + 2,)),
            pltpu.SemaphoreType.DMA((bands + 2,)),
            pltpu.SemaphoreType.DMA((5,)),
        ],
        compiler_params=pltpu.CompilerParams(collective_id=0, has_side_effects=True, vmem_limit_bytes=limit),
        name="coadd",
    )(*[
        x if x is slot_count else pltpu.with_memory_space_constraint(x, pltpu.MemorySpace.HBM)
        for x in (
            slot_count, slot_offset.T, slot_frac.T, slot_pixels, template, slot_tile.T, slot_sigma.T,
            clip_mask, prior_weight,
        )
    ])

    return pl.pallas_call(
        leave_kernel,
        out_shape=(block, block),
        in_specs=[vmem] * 2,
        out_specs=(pl.BlockSpec(memory_space=pl.ANY),) * 2,
        scratch_shapes=[pltpu.SemaphoreType.DMA((2,))],
        compiler_params=pltpu.CompilerParams(vmem_limit_bytes=1024 * 1024),
        name="leave",
    )(*results)

def solution(mesh):
    in_specs = (
        P(("groups", "sky", "epoch"), "band", None, None),
        P(("groups", "sky", "epoch"), None),
        P(("groups", "sky", "epoch"), None),
        P(("groups", "sky", "epoch"), None),
        P(("groups", "sky", "epoch"), "band"),
        P(("groups", "sky", "epoch"), None, None),
        P(("groups", "sky", "epoch")),
        P("band", ("groups", "sky"), None),
        P("band", ("groups", "sky")),
    )
    out_specs = (P("band", ("groups", "sky"), "epoch"), P("band", ("groups", "sky"), "epoch"))
    return jax.shard_map(
        on_device, mesh=mesh, in_specs=in_specs, out_specs=out_specs, check_vma=False
    )
```

```python
import functools
import math

import jax
import jax.numpy as jnp
from jax import lax
from jax.experimental import pallas as pl
from jax.experimental.pallas import tpu as pltpu
from jax.sharding import PartitionSpec as P

MARGIN = 8
BLOCK_ROWS = 8
REACH = 3
TAPS = 2 * REACH
LANES = 128
CAPACITY = 2
CLIP_WIDTH = 3.0
NOBODY = -64.0
PRIOR_PARTS = 3
AT_ONCE = 4
TILE, DY, DX, FY, FX, SIGMA = range(6)
MESH = pl.DeviceIdType.MESH
F32 = jnp.float32
BF16 = jnp.bfloat16

def sinc(x):
    at_zero = x == 0.0
    turned = math.pi * jnp.where(at_zero, 1.0, x)
    return jnp.where(at_zero, 1.0, jnp.sin(turned) / turned)

def lanczos(distance):
    inside = jnp.abs(distance) < 3.0
    return jnp.where(inside, sinc(distance) * sinc(distance / 3.0), 0.0)

def rounded(x):
    return x.astype(BF16).astype(F32)

def iota(shape, dim):
    return lax.broadcasted_iota(jnp.int32, shape, dim)

def ones_where(condition):
    return jnp.where(condition, 1.0, 0.0).astype(BF16)

def dot(a, b):
    return jnp.dot(a, b, preferred_element_type=F32)

def dot_first(a, b):
    return lax.dot_general(a, b, (((0,), (0,)), ((), ())), preferred_element_type=F32)

def between(x, extent):
    return (x >= 0.0) & (x < float(extent))

def coadd_kernel(
    shape, *refs,
):
    count_ref, *inputs = refs[:9]
    (
        coadd_ref, depth_ref,
        offset_ref, frac_ref, template_ref, tile_ref, sigma_ref, mask_ref, prior_ref,
        pixels, small, group, relay, others, tap_table, lag_ref, kernel_x, columns, columns_held, template_held,
        framed, flux, left, weigh, inverse, send, held, cover_ref,
        local_sem, message_sem, template_sem, columns_sem, flux_sem, sent_sem,
    ) = refs[9:]
    bands, sky, epochs, rows, cols, slots, blocks, mask_cols = shape
    part = cols // epochs
    canvas = rows + 2 * MARGIN
    padded = cols + LANES
    held_slots = slots + -slots % 8
    fields = SIGMA + bands
    field_at = blocks * mask_cols
    at_once = sky if sky <= AT_ONCE else 1
    pairs = at_once * CAPACITY
    me = lax.axis_index("sky")
    epoch = lax.axis_index("epoch")
    own_cols = pl.ds(pl.multiple_of(epoch * part, LANES), part)

    def sky_peer(d):
        return lax.rem(me + d, sky)

    def epoch_peer(d):
        return lax.rem(epoch + d, epochs)

    barrier = pltpu.get_barrier_semaphore()
    for d in range(1, sky):
        pl.semaphore_signal(barrier, inc=1, device_id={"sky": sky_peer(d)}, device_id_type=MESH)
    for d in range(1, epochs):
        pl.semaphore_signal(barrier, inc=1, device_id={"epoch": epoch_peer(d)}, device_id_type=MESH)
    targets = [offset_ref, frac_ref, pixels.at[0], template_ref, tile_ref, sigma_ref, mask_ref, prior_ref]
    targets += [pixels.at[b] for b in range(1, bands)]
    sources = inputs[:2] + [inputs[2].at[:, 0]] + inputs[3:] + [inputs[2].at[:, b] for b in range(1, bands)]
    loads = []
    for i, (source, target) in enumerate(zip(sources, targets)):
        loads.append(pltpu.make_async_copy(source, target, local_sem.at[i]))
        loads[-1].start()

    def remote(src, dst, sent, received, where):
        pltpu.make_async_remote_copy(
            src_ref=src, dst_ref=dst, send_sem=sent, recv_sem=received, device_id=where, device_id_type=MESH
        ).start()

    def wait_bytes(ref, sem):
        pltpu.make_async_copy(ref, ref, sem).wait()

    halves = 2 if part % (2 * LANES) == 0 else 1
    chunks = []
    for b in range(bands):
        pieces = 1
        chunks += [(b, i * (part // pieces), part // pieces) for i in range(pieces)]

    tall = (2 * LANES, LANES)
    reached = LANES + 2 * MARGIN
    source_at = jnp.where(iota(tall, 0) < 3 * LANES // 2, iota(tall, 0), iota(tall, 0) - 2 * LANES)
    lag_ref[...] = (source_at - iota(tall, 1)).astype(F32)
    idle = jnp.zeros((2 * LANES - 2 * MARGIN - reached, LANES), BF16)
    for p in range(slots):
        kernel_x[p, reached : 2 * LANES - 2 * MARGIN] = idle
    for load in loads[:2]:
        load.wait()
    tap_rows = jnp.broadcast_to(frac_ref[1:2].astype(F32), (8, slots))
    tap_rows = rounded(lanczos((REACH - iota((8, slots), 0)).astype(F32) - tap_rows))
    lag_rows = (iota((8, slots), 0) - REACH - jnp.broadcast_to(offset_ref[1:2], (8, slots))).astype(F32)
    for p in range(slots):
        tap_table[0, p] = jnp.broadcast_to(tap_rows[:, p : p + 1], (8, LANES))
        tap_table[1, p] = jnp.broadcast_to(lag_rows[:, p : p + 1], (8, LANES))
    ahead = ones_where(iota((rows, LANES), 1) < LANES // 2)
    behind = ones_where(iota((rows, LANES), 1) >= LANES // 2)

    def over_slots(step):
        lax.fori_loop(0, slots, lambda p, c: (step(p), c)[1], 0, unroll=slots <= 8)

    def build_kernel(p):
        for part_rows in (slice(0, reached), slice(2 * LANES - 2 * MARGIN, 2 * LANES)):
            lag = lag_ref[part_rows]
            total = jnp.zeros(lag.shape, F32)
            for t in range(TAPS):
                total = jnp.where(lag == tap_table[1, p, t : t + 1], tap_table[0, p, t : t + 1], total)
            kernel_x[p, part_rows] = total.astype(BF16)

    def warp_columns(b):
        def one_slot(p):
            count = cols // LANES
            source = [pixels[b, p, :, c * LANES : (c + 1) * LANES] for c in range(count)]
            blocks_in = []
            for c in range(count):
                beside = jnp.zeros((rows, LANES), BF16)
                if c + 1 < count:
                    beside = source[c + 1] * ahead
                if c:
                    beside = beside + source[c - 1] * behind
                blocks_in.append(jnp.concatenate([source[c], beside], 1))
            summed = dot(jnp.concatenate(blocks_in, 0), kernel_x[p]).astype(BF16)
            here = pl.ds(pl.multiple_of(p * rows, rows), rows)
            for c in range(count):
                e, first = c * LANES // part, c * LANES % part
                columns[e, b, here, first : first + LANES] = summed[c * rows : (c + 1) * rows]

        over_slots(one_slot)

    near_core = lax.axis_index("band") > 0

    def send_columns(i):
        if chunks[i][0] == 0:
            send_columns_now(i)
        else:
            pl.when(jnp.logical_not(near_core))(functools.partial(send_columns_now, i))

    def send_columns_now(i):
        b, first, width = chunks[i]
        at = pl.ds(first, width)
        for d in range(1, epochs):
            remote(
                columns.at[epoch_peer(d), b, :, at], columns_held.at[d - 1, b, :, at],
                sent_sem.at[0], columns_sem.at[i], {"epoch": epoch_peer(d)},
            )

    def send_template(b):
        for d in range(1, sky):
            remote(
                template_ref.at[b, :, own_cols], template_held.at[d - 1, b],
                sent_sem.at[1], template_sem.at[b], {"sky": sky_peer(d)},
            )

    over_slots(build_kernel)
    for load in loads[2:8]:
        load.wait()

    warp_columns(0)
    lane = iota((8, LANES), 1)
    small[...] = jnp.ones_like(small)
    tile = jnp.where(iota((1, slots), 1) < count_ref[0], tile_ref[...].astype(F32), NOBODY)
    small[TILE : TILE + 1] = jnp.full((1, LANES), NOBODY, F32)
    small[TILE : TILE + 1, :slots] = tile
    small[DY : DX + 1, :slots] = offset_ref[...].astype(F32)
    small[FY : FX + 1, :slots] = frac_ref[...].astype(F32)
    small[SIGMA:fields, :slots] = sigma_ref[...].astype(F32)
    by_lane = small[...]
    field_rows = by_lane.shape[0]
    place = ones_where(iota((16, LANES), 1) == iota((16, LANES), 0) + field_at)
    tall = jnp.concatenate([by_lane, jnp.zeros((16 - field_rows, LANES), F32)], 0) if field_rows < 16 else by_lane
    by_slot = dot_first(tall.astype(BF16), place[: tall.shape[0]])[:held_slots]
    cells = []
    for p in range(held_slots):
        if p < slots:
            cells.append(mask_ref[p].astype(F32))
            if blocks % 8:
                cells.append(jnp.zeros((-blocks % 8, mask_cols), F32))
        else:
            cells.append(jnp.zeros((blocks + -blocks % 8, mask_cols), F32))
    cells = jnp.concatenate(cells, 0)
    tall_blocks = blocks + -blocks % 8
    wide = (mask_cols, LANES)
    spread = ones_where((lax.rem(iota(wide, 1), mask_cols) == iota(wide, 0)) & (iota(wide, 1) < field_at))
    wide = dot(cells.astype(BF16), spread)
    wide = jnp.where(iota(wide.shape, 1) // mask_cols == lax.rem(iota(wide.shape, 0), tall_blocks), wide, 0.0)
    gather = (held_slots, held_slots * tall_blocks)
    by_slot = by_slot + dot(ones_where(iota(gather, 1) // tall_blocks == iota(gather, 0)), wide.astype(BF16))
    prior = jnp.concatenate([prior_ref[...], jnp.zeros((-bands % 8, rows), F32)], 0)
    prior = jnp.sum(prior, 1, keepdims=True)
    high = rounded(prior)
    middle = rounded(prior - high)
    prior_at = field_at + fields
    parts = jnp.where(lane == prior_at, high, 0.0) + jnp.where(lane == prior_at + 1, middle, 0.0)
    parts = parts + jnp.where(lane == prior_at + 2, prior - high - middle, 0.0)
    if held_slots > 8:
        parts = jnp.concatenate([parts, jnp.zeros((held_slots - 8, LANES), F32)], 0)
    by_slot = jnp.where(iota(by_slot.shape, 1) < prior_at, by_slot, parts)
    group[0] = jnp.concatenate([by_slot, by_lane], 0).astype(BF16)

    def column(a, f):
        return a[:, field_at + f : field_at + f + 1]

    def slot_taps(a):
        at = iota(a.shape, 1)
        fraction = jnp.where(at < 8, column(a, FX), column(a, FY))
        return rounded(lanczos((REACH - lax.rem(at, 8)).astype(F32) - fraction))

    def column_cover(a, taps, first, width):
        at = (iota((a.shape[0], width), 1) + first).astype(F32) - column(a, DX)
        total = jnp.zeros(at.shape, F32)
        for t in range(TAPS):
            total = total + jnp.where(between(at + float(t - REACH), cols), taps[:, t : t + 1], 0.0)
        return jnp.clip(total, 0.0, 1.0)

    pl.semaphore_wait(barrier, sky - 1 + epochs - 1)

    for d in range(1, epochs):
        remote(group.at[0], group.at[d], sent_sem.at[2], message_sem.at[0], {"epoch": epoch_peer(d)})
    for i, chunk in enumerate(chunks):
        if chunk[0] == 0:
            send_columns(i)
    send_template(0)
    for b in range(1, bands):

        loads[7 + b].wait()
        warp_columns(b)

        for i, chunk in enumerate(chunks):
            if chunk[0] == b:
                send_columns(i)
        send_template(b)

    flux[...] = jnp.zeros_like(flux)
    edge = jnp.zeros((bands, MARGIN, part), F32)
    framed[:, :MARGIN] = edge
    framed[:, MARGIN + sky * rows :] = edge
    own_rows = pl.ds(pl.multiple_of(MARGIN + me * rows, 8), rows)
    for b in range(bands):
        framed[b, own_rows] = template_ref[b, :, own_cols].astype(F32)

    depth_k = slots * rows
    cell_k = blocks * held_slots
    to_rows = ones_where(iota((LANES, depth_k), 1) // rows == iota((LANES, depth_k), 0))
    to_cells = (LANES, cell_k)
    to_cells = ones_where(
        (lax.rem(iota(to_cells, 1), held_slots) == iota(to_cells, 0)) & (iota(to_cells, 0) < slots)
    )

    def prepare(d, first_owner):
        message = group[d].astype(F32)
        a, by_lane = message[:held_slots], message[held_slots:]
        lanes = iota((held_slots, LANES), 1)
        same = (column(a, TILE) == by_lane[TILE : TILE + 1]) & (iota(lanes.shape, 0) < lanes)
        rank = jnp.sum(jnp.where(same, 1.0, 0.0), 0, keepdims=True)
        tap_rows = (REACH - iota((8, LANES), 0)).astype(F32) - by_lane[FY : FY + 1]
        tap_rows = rounded(lanczos(tap_rows))
        stack = jnp.concatenate(
            [tap_rows, jnp.broadcast_to(rank, (8, LANES)), by_lane] + [tap_rows] * (by_lane.shape[0] // 8 % 2), 0
        ).astype(BF16)
        k_stack = dot(stack, to_rows)
        gap = iota((canvas, depth_k), 0) - MARGIN - lax.rem(iota((canvas, depth_k), 1), rows)
        gap = gap.astype(F32) - k_stack[16 + DY : 17 + DY]
        row_table = jnp.zeros((canvas, depth_k), F32)
        for t in range(TAPS):
            row_table = row_table + jnp.where(gap == float(REACH - t), k_stack[t : t + 1], 0.0)
        c_stack = dot(stack, to_cells)
        c_lane = iota((canvas, cell_k), 1)
        reach = (iota((canvas, cell_k), 0) - MARGIN).astype(F32) - c_stack[16 + DY : 17 + DY]
        cover = jnp.zeros((canvas, cell_k), F32)
        for t in range(TAPS):
            cover = cover + jnp.where(between(reach + float(t - REACH), rows), c_stack[t : t + 1], 0.0)
        cover = jnp.clip(cover, 0.0, 1.0)
        cover = jnp.where(iota((canvas, cell_k), 0) // BLOCK_ROWS == c_lane // held_slots, cover, 0.0)
        cover = jnp.where(lax.rem(c_lane, held_slots) < slots, cover, 0.0)
        slot_cover = column_cover(a, slot_taps(a), epoch * part, part)
        chosen = [jnp.where(iota(a.shape, 1) // mask_cols == i, a, 0.0) for i in range(blocks)]
        wide = (LANES, part)
        spread = lax.rem(iota(wide, 0), mask_cols) == (iota(wide, 1) + epoch * part) // (cols // mask_cols)
        spread = ones_where(spread & (iota(wide, 0) < field_at))
        cells = dot(jnp.concatenate(chosen, 0).astype(BF16), spread)
        cells = (cells * jnp.concatenate([slot_cover] * blocks, 0)).astype(BF16)

        def here(stacked, owner, k):
            return (stacked[16 + TILE : 17 + TILE] == owner.astype(F32)) & (stacked[8:9] == float(k))

        pair_row = iota((pairs, LANES), 0)
        picked = (by_lane[TILE : TILE + 1] == (first_owner + pair_row // CAPACITY).astype(F32)) & (
            rank == lax.rem(pair_row, CAPACITY).astype(F32)
        ) & (iota((pairs, LANES), 1) < slots)
        for b in range(bands):
            scale = 1.0 / (CLIP_WIDTH * by_lane[SIGMA + b : SIGMA + b + 1])
            scale = jnp.sum(jnp.where(picked, scale, 0.0), 1, keepdims=True)
            inverse[d, b] = jnp.broadcast_to(scale, (pairs, LANES))
        sigma = [c_stack[16 + SIGMA + b : 17 + SIGMA + b] for b in range(bands)]
        weight = [cover * (CLIP_WIDTH / jnp.where(s > 0.0, s, 1.0)) for s in sigma]
        lhs = [[] for _ in range(bands)]
        for pair in range(pairs):
            owner, k = jnp.int32(first_owner + pair // CAPACITY), pair % CAPACITY
            at = slice(pair * canvas, (pair + 1) * canvas)
            left[d, at] = jnp.where(here(k_stack, owner, k), row_table, 0.0).astype(BF16)
            mine = here(c_stack, owner, k)
            for b in range(bands):
                lhs[b].append(jnp.where(mine, weight[b], 0.0))
        for b in range(bands):
            weigh[d, b] = dot(jnp.concatenate(lhs[b], 0).astype(BF16), cells)

    def process(d, chunk, first_owner):
        b, first, width = chunk
        lanes = slice(first, first + width)
        source = columns[epoch, b, :, lanes] if d == 0 else columns_held[d - 1, b, :, lanes]
        for o in range(at_once):
            at = pl.ds(pl.multiple_of((first_owner + o) * rows, 8), canvas)
            frame = framed[b, at, lanes]
            total = flux[b, at, lanes]
            both = slice(o * CAPACITY * canvas, (o + 1) * CAPACITY * canvas)
            warped = dot(left[d, both], source)
            for k in range(CAPACITY):
                pair = o * CAPACITY + k
                here = slice(pair * canvas, (pair + 1) * canvas)
                scale = jnp.concatenate([inverse[d, b, pair : pair + 1]] * (width // LANES), 1)
                total = total + weigh[d, b, here, lanes] * jnp.tanh((warped[k * canvas : (k + 1) * canvas] - frame) * scale)
            flux[b, at, lanes] = total

    def all_owners(step):
        if sky == at_once:
            step(0)
        else:
            lax.fori_loop(0, sky // at_once, lambda i, c: (step(i * at_once), c)[1], 0)

    if sky == at_once:
        prepare(0, 0)

    def send_held_back():
        for i, chunk in enumerate(chunks):
            if chunk[0] > 0:
                send_columns_now(i)

    def meet_epoch_peers():
        wait_bytes(group.at[1:], message_sem.at[0])
        relay[...] = jnp.concatenate([group[d, :held_slots] for d in range(epochs)], 0)
        for d in range(1, sky):
            remote(relay, others.at[d - 1], sent_sem.at[3], message_sem.at[1], {"sky": sky_peer(d)})
        if sky == at_once:

            for d in range(1, epochs):
                prepare(d, 0)

    meet_epoch_peers()
    for i, chunk in enumerate(chunks):
        b, first, width = chunk
        lanes = slice(first, first + width)
        if first == 0:

            wait_bytes(template_held.at[:, b], template_sem.at[b])
            for d in range(1, sky):
                at = pl.ds(pl.multiple_of(MARGIN + lax.rem(me - d + sky, sky) * rows, 8), rows)
                framed[b, at] = template_held[d - 1, b].astype(F32)
        for d in range(epochs):
            if d == 1:

                wait_bytes(columns_held.at[:, b, :, pl.ds(first, width)], columns_sem.at[i])

            def step(first_owner, d=d, chunk=chunk):
                if sky != at_once:
                    prepare(d, first_owner)
                process(d, chunk, first_owner)

            all_owners(step)
        if i == 0:
            pl.when(near_core)(send_held_back)

        for d in range(1, sky):
            at = pl.ds(pl.multiple_of(MARGIN + sky_peer(d) * rows, 8), rows)
            send[d - 1, b, :, lanes] = flux[b, at, lanes].astype(BF16)
        for d in range(1, sky):
            at = pl.ds(first, width)
            remote(
                send.at[d - 1, b, :, at], held.at[d - 1, b, :, at],
                sent_sem.at[4], flux_sem.at[i], {"sky": sky_peer(d)},
            )


    wait_bytes(others, message_sem.at[1])

    square = (LANES, LANES)
    by_block = iota(square, 0) // BLOCK_ROWS == iota(square, 1) // mask_cols
    by_block = ones_where(by_block & (iota(square, 0) < canvas) & (iota(square, 1) < field_at))
    wide = (cols, LANES)
    by_cell = ones_where(iota(wide, 0) // (cols // mask_cols) == lax.rem(iota(wide, 1), mask_cols))
    wide = (LANES, part)
    to_cols = lax.rem(iota(wide, 0), mask_cols) == (iota(wide, 1) + epoch * part) // (cols // mask_cols)
    to_cols = ones_where(to_cols)

    def depth_from(groups):
        every = jnp.concatenate([message.astype(F32) for message in groups], 0)
        prior_total = jnp.zeros((8, 1), F32)
        for message in groups:
            prior = message[:8].astype(F32)[:, prior_at : prior_at + PRIOR_PARTS]
            prior_total = prior_total + jnp.sum(prior, 1, keepdims=True)
        number = every.shape[0]
        taps = slot_taps(every)
        cover = cover_ref.at[:number]
        cover[...] = column_cover(every, taps, 0, cols)
        at = iota((number, LANES), 1)

        def row_cover(row):
            total = jnp.zeros(row.shape, F32)
            for t in range(TAPS):
                total = total + jnp.where(between(row + float(t - REACH), rows), taps[:, 8 + t : 9 + t], 0.0)
            return jnp.clip(total, 0.0, 1.0)

        tile = column(every, TILE)
        row = (at - MARGIN).astype(F32)
        canvas_cover = row_cover(row - column(every, DY))
        in_patch = between(row + tile * float(rows), sky * rows) & (at < canvas)
        canvas_cover = jnp.where(in_patch, canvas_cover, 0.0)
        area = dot(canvas_cover.astype(BF16), by_block) * dot(cover[...].astype(BF16), by_cell)
        area = jnp.where(at < field_at, every * area, 0.0)
        area = jnp.sum(area, 1, keepdims=True)
        precision = [1.0 / (column(every, SIGMA + b) * column(every, SIGMA + b)) for b in range(bands)]
        totals = []
        for b in range(bands):
            total = jnp.sum(area * jnp.where(tile >= 0.0, precision[b], 0.0), 0, keepdims=True)
            totals.append(total + prior_total[b : b + 1] * float(cols))
        group_rows = rows // BLOCK_ROWS
        wide = (number, bands * rows)
        in_band = iota(wide, 1)
        row = (lax.rem(in_band, rows) + me * rows).astype(F32) - tile * float(rows) - column(every, DY)
        profile = row_cover(row)
        factor = jnp.zeros(wide, F32)
        for b in range(bands):
            factor = jnp.where(in_band // rows == b, precision[b], factor)
        profile = profile * factor
        block = lax.rem(in_band, rows) // BLOCK_ROWS
        lhs = jnp.concatenate([jnp.where(block == g, profile, 0.0) for g in range(group_rows)], 0).astype(BF16)
        first = MARGIN // BLOCK_ROWS
        canvas_block = (first + group_rows * me).astype(F32) - tile * float(group_rows)
        chosen = [
            jnp.where(((at // mask_cols).astype(F32) == canvas_block + float(g)) & (at < field_at), every, 0.0)
            for g in range(group_rows)
        ]
        cells = dot(jnp.concatenate(chosen, 0).astype(BF16), to_cols)
        own_cover = cover[:, own_cols]
        cells = (cells * jnp.concatenate([own_cover] * group_rows, 0)).astype(BF16)
        return (dot_first(lhs, cells), *totals)

    if sky <= AT_ONCE:
        weights, *totals = depth_from([relay[...]] + [others[d - 1] for d in range(1, sky)])
    else:
        weights, *totals = lax.fori_loop(
            0, sky - 1,
            lambda d, sums: tuple(x + y for x, y in zip(sums, depth_from([others[d]]))),
            depth_from([relay[...]]),
        )
    means = [total * (1.0 / (sky * rows * cols)) for total in totals]
    diagonal = iota((rows, rows), 0) == iota((rows, rows), 1)
    depths = []
    for b in range(bands):
        prior = jnp.sum(jnp.where(diagonal, prior_ref[b : b + 1], 0.0), 1, keepdims=True)
        depth = weights[b * rows : (b + 1) * rows] + prior
        depth_ref[b] = (depth / means[b]).astype(BF16)
        depths.append(depth)

    for sent, ref in enumerate((columns_held, template_held, group.at[1:], others)):
        wait_bytes(ref, sent_sem.at[sent])
    for i, (b, first, width) in enumerate(chunks):
        lanes = slice(first, first + width)

        wait_bytes(held.at[:, b, :, pl.ds(first, width)], flux_sem.at[i])

        total = flux[b, own_rows, lanes]
        for d in range(1, sky):
            total = total + held[d - 1, b, :, lanes].astype(F32)
        coadd_ref[b, :, lanes] = (framed[b, own_rows, lanes] + total / depths[b][:, lanes]).astype(BF16)

    wait_bytes(send, sent_sem.at[4])

def leave_kernel(coadd_in, depth_in, coadd_ref, depth_ref, sem):
    copies = [
        pltpu.make_async_copy(coadd_in, coadd_ref, sem.at[0]),
        pltpu.make_async_copy(depth_in, depth_ref, sem.at[1]),
    ]
    for copy in copies:
        copy.start()
    for copy in copies:
        copy.wait()

def on_device(
    slot_pixels, slot_tile, slot_offset, slot_frac, slot_sigma, clip_mask, slot_count, template, prior_weight
):
    sky = lax.axis_size("sky")
    epochs = lax.axis_size("epoch")
    slots, bands, rows, cols = slot_pixels.shape
    blocks, mask_cols = clip_mask.shape[1:]
    part = cols // epochs
    canvas = rows + 2 * MARGIN
    held_slots = slots + -slots % 8
    field_rows = SIGMA + bands + -(SIGMA + bands) % 8
    message = held_slots + field_rows
    at_once = sky if sky <= AT_ONCE else 1
    pairs = at_once * CAPACITY
    vmem = pl.BlockSpec(memory_space=pltpu.VMEM)
    block = jax.ShapeDtypeStruct((bands, rows, part), BF16)
    patch = sky * rows + 2 * MARGIN
    limit = 32 * 1024 * 1024 if sky <= AT_ONCE else None
    results = pl.pallas_call(
        functools.partial(coadd_kernel, (bands, sky, epochs, rows, cols, slots, blocks, mask_cols)),
        out_shape=(block, block),
        in_specs=[pl.BlockSpec(memory_space=pltpu.SMEM)] + [pl.BlockSpec(memory_space=pltpu.MemorySpace.HBM)] * 8,
        out_specs=(vmem, vmem),
        scratch_shapes=[
            pltpu.VMEM((2, slots), jnp.int32),
            pltpu.VMEM((2, slots), BF16),
            pltpu.VMEM((bands, rows, cols), BF16),
            pltpu.VMEM((1, slots), jnp.int32),
            pltpu.VMEM((bands, slots), BF16),
            pltpu.VMEM((slots, blocks, mask_cols), jnp.int32),
            pltpu.VMEM((bands, rows), F32),
            pltpu.VMEM((bands, slots, rows, cols), BF16),
            pltpu.VMEM((field_rows, LANES), F32),
            pltpu.VMEM((epochs, message, LANES), BF16),
            pltpu.VMEM((epochs * held_slots, LANES), BF16),
            pltpu.VMEM((sky - 1, epochs * held_slots, LANES), BF16),
            pltpu.VMEM((2, slots, 8, LANES), F32),
            pltpu.VMEM((2 * LANES, LANES), F32),
            pltpu.VMEM((slots, 2 * LANES, LANES), BF16),
            pltpu.VMEM((epochs, bands, slots * rows, part), BF16),
            pltpu.VMEM((epochs - 1, bands, slots * rows, part), BF16),
            pltpu.VMEM((sky - 1, bands, rows, part), BF16),
            pltpu.VMEM((bands, patch, part), F32),
            pltpu.VMEM((bands, patch, part), F32),
            pltpu.VMEM((epochs, pairs * canvas, slots * rows), BF16),
            pltpu.VMEM((epochs, bands, pairs * canvas, part), F32),
            pltpu.VMEM((epochs, bands, pairs, LANES), F32),
            pltpu.VMEM((sky - 1, bands, rows, part), BF16),
            pltpu.VMEM((sky - 1, bands, rows, part), BF16),
            pltpu.VMEM(((sky if sky <= AT_ONCE else 1) * epochs * held_slots, cols), F32),
            pltpu.SemaphoreType.DMA((bands + 7,)),
            pltpu.SemaphoreType.DMA((2,)),
            pltpu.SemaphoreType.DMA((bands,)),
            pltpu.SemaphoreType.DMA((bands + 2,)),
            pltpu.SemaphoreType.DMA((bands + 2,)),
            pltpu.SemaphoreType.DMA((5,)),
        ],
        compiler_params=pltpu.CompilerParams(collective_id=0, has_side_effects=True, vmem_limit_bytes=limit),
        name="coadd",
    )(*[
        x if x is slot_count else pltpu.with_memory_space_constraint(x, pltpu.MemorySpace.HBM)
        for x in (
            slot_count, slot_offset.T, slot_frac.T, slot_pixels, template, slot_tile.T, slot_sigma.T,
            clip_mask, prior_weight,
        )
    ])

    return pl.pallas_call(
        leave_kernel,
        out_shape=(block, block),
        in_specs=[vmem] * 2,
        out_specs=(pl.BlockSpec(memory_space=pl.ANY),) * 2,
        scratch_shapes=[pltpu.SemaphoreType.DMA((2,))],
        compiler_params=pltpu.CompilerParams(vmem_limit_bytes=1024 * 1024),
        name="leave",
    )(*results)

def solution(mesh):
    in_specs = (
        P(("groups", "sky", "epoch"), "band", None, None),
        P(("groups", "sky", "epoch"), None),
        P(("groups", "sky", "epoch"), None),
        P(("groups", "sky", "epoch"), None),
        P(("groups", "sky", "epoch"), "band"),
        P(("groups", "sky", "epoch"), None, None),
        P(("groups", "sky", "epoch")),
        P("band", ("groups", "sky"), None),
        P("band", ("groups", "sky")),
    )
    out_specs = (P("band", ("groups", "sky"), "epoch"), P("band", ("groups", "sky"), "epoch"))
    return jax.shard_map(
        on_device, mesh=mesh, in_specs=in_specs, out_specs=out_specs, check_vma=False
    )
```

```python
import functools
import math

import jax
import jax.numpy as jnp
from jax import lax
from jax.experimental import pallas as pl
from jax.experimental.pallas import tpu as pltpu
from jax.sharding import PartitionSpec as P

MARGIN = 8
BLOCK_ROWS = 8
REACH = 3
TAPS = 2 * REACH
LANES = 128
CAPACITY = 2
CLIP_WIDTH = 3.0
NOBODY = -64.0
PRIOR_PARTS = 3
AT_ONCE = 4
TILE, DY, DX, FY, FX, SIGMA = range(6)
MESH = pl.DeviceIdType.MESH
F32 = jnp.float32
BF16 = jnp.bfloat16

def sinc(x):
    at_zero = x == 0.0
    turned = math.pi * jnp.where(at_zero, 1.0, x)
    return jnp.where(at_zero, 1.0, jnp.sin(turned) / turned)

def lanczos(distance):
    inside = jnp.abs(distance) < 3.0
    return jnp.where(inside, sinc(distance) * sinc(distance / 3.0), 0.0)

def rounded(x):
    return x.astype(BF16).astype(F32)

def iota(shape, dim):
    return lax.broadcasted_iota(jnp.int32, shape, dim)

def ones_where(condition):
    return jnp.where(condition, 1.0, 0.0).astype(BF16)

def dot(a, b):
    return jnp.dot(a, b, preferred_element_type=F32)

def dot_first(a, b):
    return lax.dot_general(a, b, (((0,), (0,)), ((), ())), preferred_element_type=F32)

def between(x, extent):
    return (x >= 0.0) & (x < float(extent))

def coadd_kernel(
    shape, *refs,
):
    count_ref, *inputs = refs[:9]
    (
        coadd_ref, depth_ref,
        offset_ref, frac_ref, template_ref, tile_ref, sigma_ref, mask_ref, prior_ref,
        pixels, small, group, relay, others, tap_table, lag_ref, kernel_x, columns, columns_held, template_held,
        framed, flux, left, weigh, inverse, send, held, cover_ref,
        local_sem, message_sem, template_sem, columns_sem, flux_sem, sent_sem,
    ) = refs[9:]
    bands, sky, epochs, rows, cols, slots, blocks, mask_cols = shape
    part = cols // epochs
    canvas = rows + 2 * MARGIN
    padded = cols + LANES
    held_slots = slots + -slots % 8
    fields = SIGMA + bands
    field_at = blocks * mask_cols
    at_once = sky if sky <= AT_ONCE else 1
    pairs = at_once * CAPACITY
    me = lax.axis_index("sky")
    epoch = lax.axis_index("epoch")
    own_cols = pl.ds(pl.multiple_of(epoch * part, LANES), part)

    def sky_peer(d):
        return lax.rem(me + d, sky)

    far_order = [jnp.where(me < sky // 2, sky - k, k) for k in range(1, sky)]

    def epoch_peer(d):
        return lax.rem(epoch + d, epochs)

    barrier = pltpu.get_barrier_semaphore()
    for d in range(1, sky):
        pl.semaphore_signal(barrier, inc=1, device_id={"sky": sky_peer(d)}, device_id_type=MESH)
    for d in range(1, epochs):
        pl.semaphore_signal(barrier, inc=1, device_id={"epoch": epoch_peer(d)}, device_id_type=MESH)
    targets = [offset_ref, frac_ref, pixels.at[0], template_ref, tile_ref, sigma_ref, mask_ref, prior_ref]
    targets += [pixels.at[b] for b in range(1, bands)]
    sources = inputs[:2] + [inputs[2].at[:, 0]] + inputs[3:] + [inputs[2].at[:, b] for b in range(1, bands)]
    loads = []
    for i, (source, target) in enumerate(zip(sources, targets)):
        sem = sent_sem.at[i] if i < 5 else local_sem.at[i - 5]
        loads.append(pltpu.make_async_copy(source, target, sem))
        loads[-1].start()

    def remote(src, dst, sent, received, where):
        pltpu.make_async_remote_copy(
            src_ref=src, dst_ref=dst, send_sem=sent, recv_sem=received, device_id=where, device_id_type=MESH
        ).start()

    def wait_bytes(ref, sem):
        pltpu.make_async_copy(ref, ref, sem).wait()

    halves = 2 if part % (2 * LANES) == 0 else 1
    chunks = []
    for b in range(bands):
        pieces = halves if b == bands - 1 else 1
        chunks += [(b, i * (part // pieces), part // pieces) for i in range(pieces)]

    tall = (2 * LANES, LANES)
    reached = LANES + 2 * MARGIN
    source_at = jnp.where(iota(tall, 0) < 3 * LANES // 2, iota(tall, 0), iota(tall, 0) - 2 * LANES)
    lag_ref[...] = (source_at - iota(tall, 1)).astype(F32)
    idle = jnp.zeros((2 * LANES - 2 * MARGIN - reached, LANES), BF16)
    for p in range(slots):
        kernel_x[p, reached : 2 * LANES - 2 * MARGIN] = idle
    for load in loads[:2]:
        load.wait()
    tap_rows = jnp.broadcast_to(frac_ref[1:2].astype(F32), (8, slots))
    tap_rows = rounded(lanczos((REACH - iota((8, slots), 0)).astype(F32) - tap_rows))
    lag_rows = (iota((8, slots), 0) - REACH - jnp.broadcast_to(offset_ref[1:2], (8, slots))).astype(F32)
    for p in range(slots):
        tap_table[0, p] = jnp.broadcast_to(tap_rows[:, p : p + 1], (8, LANES))
        tap_table[1, p] = jnp.broadcast_to(lag_rows[:, p : p + 1], (8, LANES))
    ahead = ones_where(iota((rows, LANES), 1) < LANES // 2)
    behind = ones_where(iota((rows, LANES), 1) >= LANES // 2)

    def over_slots(step):
        lax.fori_loop(0, slots, lambda p, c: (step(p), c)[1], 0, unroll=slots <= 8)

    def build_kernel(p):
        for part_rows in (slice(0, reached), slice(2 * LANES - 2 * MARGIN, 2 * LANES)):
            lag = lag_ref[part_rows]
            total = jnp.zeros(lag.shape, F32)
            for t in range(TAPS):
                total = jnp.where(lag == tap_table[1, p, t : t + 1], tap_table[0, p, t : t + 1], total)
            kernel_x[p, part_rows] = total.astype(BF16)

    def warp_columns(b):
        def one_slot(p):
            count = cols // LANES
            source = [pixels[b, p, :, c * LANES : (c + 1) * LANES] for c in range(count)]
            blocks_in = []
            for c in range(count):
                beside = jnp.zeros((rows, LANES), BF16)
                if c + 1 < count:
                    beside = source[c + 1] * ahead
                if c:
                    beside = beside + source[c - 1] * behind
                blocks_in.append(jnp.concatenate([source[c], beside], 1))
            summed = dot(jnp.concatenate(blocks_in, 0), kernel_x[p]).astype(BF16)
            here = pl.ds(pl.multiple_of(p * rows, rows), rows)
            for c in range(count):
                e, first = c * LANES // part, c * LANES % part
                columns[e, b, here, first : first + LANES] = summed[c * rows : (c + 1) * rows]

        over_slots(one_slot)

    near_core = lax.axis_index("band") > 0

    def send_columns(i):
        if chunks[i][0] == 0:
            send_columns_now(i)
        else:
            pl.when(jnp.logical_not(near_core))(functools.partial(send_columns_now, i))

    def send_columns_now(i):
        b, first, width = chunks[i]
        at = pl.ds(first, width)
        for d in range(1, epochs):
            remote(
                columns.at[epoch_peer(d), b, :, at], columns_held.at[d - 1, b, :, at],
                sent_sem.at[0], columns_sem.at[i], {"epoch": epoch_peer(d)},
            )

    def send_template(b):
        for d in range(1, sky):
            remote(
                template_ref.at[b, :, own_cols], template_held.at[d - 1, b],
                sent_sem.at[1], template_sem.at[b], {"sky": sky_peer(d)},
            )

    over_slots(build_kernel)
    for load in loads[2:8]:
        load.wait()

    warp_columns(0)
    lane = iota((8, LANES), 1)
    small[...] = jnp.ones_like(small)
    tile = jnp.where(iota((1, slots), 1) < count_ref[0], tile_ref[...].astype(F32), NOBODY)
    small[TILE : TILE + 1] = jnp.full((1, LANES), NOBODY, F32)
    small[TILE : TILE + 1, :slots] = tile
    small[DY : DX + 1, :slots] = offset_ref[...].astype(F32)
    small[FY : FX + 1, :slots] = frac_ref[...].astype(F32)
    small[SIGMA:fields, :slots] = sigma_ref[...].astype(F32)
    by_lane = small[...]
    field_rows = by_lane.shape[0]
    place = ones_where(iota((16, LANES), 1) == iota((16, LANES), 0) + field_at)
    tall = jnp.concatenate([by_lane, jnp.zeros((16 - field_rows, LANES), F32)], 0) if field_rows < 16 else by_lane
    by_slot = dot_first(tall.astype(BF16), place[: tall.shape[0]])[:held_slots]
    cells = []
    for p in range(held_slots):
        if p < slots:
            cells.append(mask_ref[p].astype(F32))
            if blocks % 8:
                cells.append(jnp.zeros((-blocks % 8, mask_cols), F32))
        else:
            cells.append(jnp.zeros((blocks + -blocks % 8, mask_cols), F32))
    cells = jnp.concatenate(cells, 0)
    tall_blocks = blocks + -blocks % 8
    wide = (mask_cols, LANES)
    spread = ones_where((lax.rem(iota(wide, 1), mask_cols) == iota(wide, 0)) & (iota(wide, 1) < field_at))
    wide = dot(cells.astype(BF16), spread)
    wide = jnp.where(iota(wide.shape, 1) // mask_cols == lax.rem(iota(wide.shape, 0), tall_blocks), wide, 0.0)
    gather = (held_slots, held_slots * tall_blocks)
    by_slot = by_slot + dot(ones_where(iota(gather, 1) // tall_blocks == iota(gather, 0)), wide.astype(BF16))
    prior = jnp.concatenate([prior_ref[...], jnp.zeros((-bands % 8, rows), F32)], 0)
    prior = jnp.sum(prior, 1, keepdims=True)
    high = rounded(prior)
    middle = rounded(prior - high)
    prior_at = field_at + fields
    parts = jnp.where(lane == prior_at, high, 0.0) + jnp.where(lane == prior_at + 1, middle, 0.0)
    parts = parts + jnp.where(lane == prior_at + 2, prior - high - middle, 0.0)
    if held_slots > 8:
        parts = jnp.concatenate([parts, jnp.zeros((held_slots - 8, LANES), F32)], 0)
    by_slot = jnp.where(iota(by_slot.shape, 1) < prior_at, by_slot, parts)
    group[0] = jnp.concatenate([by_slot, by_lane], 0).astype(BF16)

    def column(a, f):
        return a[:, field_at + f : field_at + f + 1]

    def slot_taps(a):
        at = iota(a.shape, 1)
        fraction = jnp.where(at < 8, column(a, FX), column(a, FY))
        return rounded(lanczos((REACH - lax.rem(at, 8)).astype(F32) - fraction))

    def column_cover(a, taps, first, width):
        at = (iota((a.shape[0], width), 1) + first).astype(F32) - column(a, DX)
        total = jnp.zeros(at.shape, F32)
        for t in range(TAPS):
            total = total + jnp.where(between(at + float(t - REACH), cols), taps[:, t : t + 1], 0.0)
        return jnp.clip(total, 0.0, 1.0)

    pl.semaphore_wait(barrier, sky - 1 + epochs - 1)

    for d in range(1, epochs):
        remote(group.at[0], group.at[d], sent_sem.at[2], message_sem.at[0], {"epoch": epoch_peer(d)})
    for i, chunk in enumerate(chunks):
        if chunk[0] == 0:
            send_columns(i)
    send_template(0)
    for b in range(1, bands):

        loads[7 + b].wait()
        warp_columns(b)

        for i, chunk in enumerate(chunks):
            if chunk[0] == b:
                send_columns(i)
        send_template(b)

    flux[...] = jnp.zeros_like(flux)
    edge = jnp.zeros((bands, MARGIN, part), F32)
    framed[:, :MARGIN] = edge
    framed[:, MARGIN + sky * rows :] = edge
    own_rows = pl.ds(pl.multiple_of(MARGIN + me * rows, 8), rows)
    for b in range(bands):
        framed[b, own_rows] = template_ref[b, :, own_cols].astype(F32)

    depth_k = slots * rows
    cell_k = blocks * held_slots
    to_rows = ones_where(iota((LANES, depth_k), 1) // rows == iota((LANES, depth_k), 0))
    to_cells = (LANES, cell_k)
    to_cells = ones_where(
        (lax.rem(iota(to_cells, 1), held_slots) == iota(to_cells, 0)) & (iota(to_cells, 0) < slots)
    )

    def prepare(d, first_owner):
        message = group[d].astype(F32)
        a, by_lane = message[:held_slots], message[held_slots:]
        lanes = iota((held_slots, LANES), 1)
        same = (column(a, TILE) == by_lane[TILE : TILE + 1]) & (iota(lanes.shape, 0) < lanes)
        rank = jnp.sum(jnp.where(same, 1.0, 0.0), 0, keepdims=True)
        tap_rows = (REACH - iota((8, LANES), 0)).astype(F32) - by_lane[FY : FY + 1]
        tap_rows = rounded(lanczos(tap_rows))
        stack = jnp.concatenate(
            [tap_rows, jnp.broadcast_to(rank, (8, LANES)), by_lane] + [tap_rows] * (by_lane.shape[0] // 8 % 2), 0
        ).astype(BF16)
        k_stack = dot(stack, to_rows)
        gap = iota((canvas, depth_k), 0) - MARGIN - lax.rem(iota((canvas, depth_k), 1), rows)
        gap = gap.astype(F32) - k_stack[16 + DY : 17 + DY]
        row_table = jnp.zeros((canvas, depth_k), F32)
        for t in range(TAPS):
            row_table = row_table + jnp.where(gap == float(REACH - t), k_stack[t : t + 1], 0.0)
        c_stack = dot(stack, to_cells)
        c_lane = iota((canvas, cell_k), 1)
        reach = (iota((canvas, cell_k), 0) - MARGIN).astype(F32) - c_stack[16 + DY : 17 + DY]
        cover = jnp.zeros((canvas, cell_k), F32)
        for t in range(TAPS):
            cover = cover + jnp.where(between(reach + float(t - REACH), rows), c_stack[t : t + 1], 0.0)
        cover = jnp.clip(cover, 0.0, 1.0)
        cover = jnp.where(iota((canvas, cell_k), 0) // BLOCK_ROWS == c_lane // held_slots, cover, 0.0)
        cover = jnp.where(lax.rem(c_lane, held_slots) < slots, cover, 0.0)
        slot_cover = column_cover(a, slot_taps(a), epoch * part, part)
        chosen = [jnp.where(iota(a.shape, 1) // mask_cols == i, a, 0.0) for i in range(blocks)]
        wide = (LANES, part)
        spread = lax.rem(iota(wide, 0), mask_cols) == (iota(wide, 1) + epoch * part) // (cols // mask_cols)
        spread = ones_where(spread & (iota(wide, 0) < field_at))
        cells = dot(jnp.concatenate(chosen, 0).astype(BF16), spread)
        cells = (cells * jnp.concatenate([slot_cover] * blocks, 0)).astype(BF16)

        def here(stacked, owner, k):
            return (stacked[16 + TILE : 17 + TILE] == owner.astype(F32)) & (stacked[8:9] == float(k))

        pair_row = iota((pairs, LANES), 0)
        picked = (by_lane[TILE : TILE + 1] == (first_owner + pair_row // CAPACITY).astype(F32)) & (
            rank == lax.rem(pair_row, CAPACITY).astype(F32)
        ) & (iota((pairs, LANES), 1) < slots)
        for b in range(bands):
            scale = 1.0 / (CLIP_WIDTH * by_lane[SIGMA + b : SIGMA + b + 1])
            scale = jnp.sum(jnp.where(picked, scale, 0.0), 1, keepdims=True)
            inverse[d, b] = jnp.broadcast_to(scale, (pairs, LANES))
        sigma = [c_stack[16 + SIGMA + b : 17 + SIGMA + b] for b in range(bands)]
        weight = [cover * (CLIP_WIDTH / jnp.where(s > 0.0, s, 1.0)) for s in sigma]
        lhs = [[] for _ in range(bands)]
        for pair in range(pairs):
            owner, k = jnp.int32(first_owner + pair // CAPACITY), pair % CAPACITY
            at = slice(pair * canvas, (pair + 1) * canvas)
            left[d, at] = jnp.where(here(k_stack, owner, k), row_table, 0.0).astype(BF16)
            mine = here(c_stack, owner, k)
            for b in range(bands):
                lhs[b].append(jnp.where(mine, weight[b], 0.0))
        for b in range(bands):
            weigh[d, b] = dot(jnp.concatenate(lhs[b], 0).astype(BF16), cells)

    def process(d, chunk, first_owner):
        b, first, width = chunk
        lanes = slice(first, first + width)
        source = columns[epoch, b, :, lanes] if d == 0 else columns_held[d - 1, b, :, lanes]
        for o in range(at_once):
            at = pl.ds(pl.multiple_of((first_owner + o) * rows, 8), canvas)
            frame = framed[b, at, lanes]
            total = flux[b, at, lanes]
            both = slice(o * CAPACITY * canvas, (o + 1) * CAPACITY * canvas)
            warped = dot(left[d, both], source)
            for k in range(CAPACITY):
                pair = o * CAPACITY + k
                here = slice(pair * canvas, (pair + 1) * canvas)
                scale = jnp.concatenate([inverse[d, b, pair : pair + 1]] * (width // LANES), 1)
                total = total + weigh[d, b, here, lanes] * jnp.tanh((warped[k * canvas : (k + 1) * canvas] - frame) * scale)
            flux[b, at, lanes] = total

    def all_owners(step):
        if sky == at_once:
            step(0)
        else:
            lax.fori_loop(0, sky // at_once, lambda i, c: (step(i * at_once), c)[1], 0)

    if sky == at_once:
        prepare(0, 0)

    def send_held_back(bands_of):
        for i, chunk in enumerate(chunks):
            if chunk[0] in bands_of:
                send_columns_now(i)

    def meet_epoch_peers():
        wait_bytes(group.at[1:], message_sem.at[0])
        relay[...] = jnp.concatenate([group[d, :held_slots] for d in range(epochs)], 0)
        for d in range(1, sky):
            remote(relay, others.at[d - 1], sent_sem.at[3], message_sem.at[1], {"sky": sky_peer(d)})
        if sky == at_once:

            for d in range(1, epochs):
                prepare(d, 0)

    meet_epoch_peers()
    for i, chunk in enumerate(chunks):
        b, first, width = chunk
        lanes = slice(first, first + width)
        if first == 0:

            wait_bytes(template_held.at[:, b], template_sem.at[b])
            for d in range(1, sky):
                at = pl.ds(pl.multiple_of(MARGIN + lax.rem(me - d + sky, sky) * rows, 8), rows)
                framed[b, at] = template_held[d - 1, b].astype(F32)
        for d in range(epochs):
            if d == 1:
                if i == 1:
                    pl.when(near_core)(functools.partial(send_held_back, range(2, bands)))

                wait_bytes(columns_held.at[:, b, :, pl.ds(first, width)], columns_sem.at[i])

            def step(first_owner, d=d, chunk=chunk):
                if sky != at_once:
                    prepare(d, first_owner)
                process(d, chunk, first_owner)

            all_owners(step)
        if i == 0:
            pl.when(near_core)(functools.partial(send_held_back, (1,)))

        for d in range(1, sky):
            at = pl.ds(pl.multiple_of(MARGIN + sky_peer(d) * rows, 8), rows)
            send[d - 1, b, :, lanes] = flux[b, at, lanes].astype(BF16)
        for d in far_order:
            at = pl.ds(first, width)
            remote(
                send.at[d - 1, b, :, at], held.at[d - 1, b, :, at],
                sent_sem.at[4], flux_sem.at[i], {"sky": sky_peer(d)},
            )


    wait_bytes(others, message_sem.at[1])

    square = (LANES, LANES)
    by_block = iota(square, 0) // BLOCK_ROWS == iota(square, 1) // mask_cols
    by_block = ones_where(by_block & (iota(square, 0) < canvas) & (iota(square, 1) < field_at))
    wide = (cols, LANES)
    by_cell = ones_where(iota(wide, 0) // (cols // mask_cols) == lax.rem(iota(wide, 1), mask_cols))
    wide = (LANES, part)
    to_cols = lax.rem(iota(wide, 0), mask_cols) == (iota(wide, 1) + epoch * part) // (cols // mask_cols)
    to_cols = ones_where(to_cols)

    def depth_from(groups):
        every = jnp.concatenate([message.astype(F32) for message in groups], 0)
        prior_total = jnp.zeros((8, 1), F32)
        for message in groups:
            prior = message[:8].astype(F32)[:, prior_at : prior_at + PRIOR_PARTS]
            prior_total = prior_total + jnp.sum(prior, 1, keepdims=True)
        number = every.shape[0]
        taps = slot_taps(every)
        cover = cover_ref.at[:number]
        cover[...] = column_cover(every, taps, 0, cols)
        at = iota((number, LANES), 1)

        def row_cover(row):
            total = jnp.zeros(row.shape, F32)
            for t in range(TAPS):
                total = total + jnp.where(between(row + float(t - REACH), rows), taps[:, 8 + t : 9 + t], 0.0)
            return jnp.clip(total, 0.0, 1.0)

        tile = column(every, TILE)
        row = (at - MARGIN).astype(F32)
        canvas_cover = row_cover(row - column(every, DY))
        in_patch = between(row + tile * float(rows), sky * rows) & (at < canvas)
        canvas_cover = jnp.where(in_patch, canvas_cover, 0.0)
        area = dot(canvas_cover.astype(BF16), by_block) * dot(cover[...].astype(BF16), by_cell)
        area = jnp.where(at < field_at, every * area, 0.0)
        area = jnp.sum(area, 1, keepdims=True)
        precision = [1.0 / (column(every, SIGMA + b) * column(every, SIGMA + b)) for b in range(bands)]
        totals = []
        for b in range(bands):
            total = jnp.sum(area * jnp.where(tile >= 0.0, precision[b], 0.0), 0, keepdims=True)
            totals.append(total + prior_total[b : b + 1] * float(cols))
        group_rows = rows // BLOCK_ROWS
        wide = (number, bands * rows)
        in_band = iota(wide, 1)
        row = (lax.rem(in_band, rows) + me * rows).astype(F32) - tile * float(rows) - column(every, DY)
        profile = row_cover(row)
        factor = jnp.zeros(wide, F32)
        for b in range(bands):
            factor = jnp.where(in_band // rows == b, precision[b], factor)
        profile = profile * factor
        block = lax.rem(in_band, rows) // BLOCK_ROWS
        lhs = jnp.concatenate([jnp.where(block == g, profile, 0.0) for g in range(group_rows)], 0).astype(BF16)
        first = MARGIN // BLOCK_ROWS
        canvas_block = (first + group_rows * me).astype(F32) - tile * float(group_rows)
        chosen = [
            jnp.where(((at // mask_cols).astype(F32) == canvas_block + float(g)) & (at < field_at), every, 0.0)
            for g in range(group_rows)
        ]
        cells = dot(jnp.concatenate(chosen, 0).astype(BF16), to_cols)
        own_cover = cover[:, own_cols]
        cells = (cells * jnp.concatenate([own_cover] * group_rows, 0)).astype(BF16)
        return (dot_first(lhs, cells), *totals)

    if sky <= AT_ONCE:
        weights, *totals = depth_from([relay[...]] + [others[d - 1] for d in range(1, sky)])
    else:
        weights, *totals = lax.fori_loop(
            0, sky - 1,
            lambda d, sums: tuple(x + y for x, y in zip(sums, depth_from([others[d]]))),
            depth_from([relay[...]]),
        )
    means = [total * (1.0 / (sky * rows * cols)) for total in totals]
    diagonal = iota((rows, rows), 0) == iota((rows, rows), 1)
    depths = []
    for b in range(bands):
        prior = jnp.sum(jnp.where(diagonal, prior_ref[b : b + 1], 0.0), 1, keepdims=True)
        depth = weights[b * rows : (b + 1) * rows] + prior
        depth_ref[b] = (depth / means[b]).astype(BF16)
        depths.append(depth)

    for sent, ref in enumerate((columns_held, template_held, group.at[1:], others)):
        wait_bytes(ref, sent_sem.at[sent])
    for i, (b, first, width) in enumerate(chunks):
        lanes = slice(first, first + width)

        wait_bytes(held.at[:, b, :, pl.ds(first, width)], flux_sem.at[i])

        total = flux[b, own_rows, lanes]
        for d in range(1, sky):
            total = total + held[d - 1, b, :, lanes].astype(F32)
        coadd_ref[b, :, lanes] = (framed[b, own_rows, lanes] + total / depths[b][:, lanes]).astype(BF16)

    wait_bytes(send, sent_sem.at[4])

def leave_kernel(coadd_in, depth_in, coadd_ref, depth_ref, sem):
    copies = [
        pltpu.make_async_copy(coadd_in, coadd_ref, sem.at[0]),
        pltpu.make_async_copy(depth_in, depth_ref, sem.at[1]),
    ]
    for copy in copies:
        copy.start()
    for copy in copies:
        copy.wait()

def on_device(
    slot_pixels, slot_tile, slot_offset, slot_frac, slot_sigma, clip_mask, slot_count, template, prior_weight
):
    sky = lax.axis_size("sky")
    epochs = lax.axis_size("epoch")
    slots, bands, rows, cols = slot_pixels.shape
    blocks, mask_cols = clip_mask.shape[1:]
    part = cols // epochs
    canvas = rows + 2 * MARGIN
    held_slots = slots + -slots % 8
    field_rows = SIGMA + bands + -(SIGMA + bands) % 8
    message = held_slots + field_rows
    at_once = sky if sky <= AT_ONCE else 1
    pairs = at_once * CAPACITY
    vmem = pl.BlockSpec(memory_space=pltpu.VMEM)
    block = jax.ShapeDtypeStruct((bands, rows, part), BF16)
    patch = sky * rows + 2 * MARGIN
    limit = 32 * 1024 * 1024 if sky <= AT_ONCE else None
    results = pl.pallas_call(
        functools.partial(coadd_kernel, (bands, sky, epochs, rows, cols, slots, blocks, mask_cols)),
        out_shape=(block, block),
        in_specs=[pl.BlockSpec(memory_space=pltpu.SMEM)] + [pl.BlockSpec(memory_space=pltpu.MemorySpace.HBM)] * 8,
        out_specs=(vmem, vmem),
        scratch_shapes=[
            pltpu.VMEM((2, slots), jnp.int32),
            pltpu.VMEM((2, slots), BF16),
            pltpu.VMEM((bands, rows, cols), BF16),
            pltpu.VMEM((1, slots), jnp.int32),
            pltpu.VMEM((bands, slots), BF16),
            pltpu.VMEM((slots, blocks, mask_cols), jnp.int32),
            pltpu.VMEM((bands, rows), F32),
            pltpu.VMEM((bands, slots, rows, cols), BF16),
            pltpu.VMEM((field_rows, LANES), F32),
            pltpu.VMEM((epochs, message, LANES), BF16),
            pltpu.VMEM((epochs * held_slots, LANES), BF16),
            pltpu.VMEM((sky - 1, epochs * held_slots, LANES), BF16),
            pltpu.VMEM((2, slots, 8, LANES), F32),
            pltpu.VMEM((2 * LANES, LANES), F32),
            pltpu.VMEM((slots, 2 * LANES, LANES), BF16),
            pltpu.VMEM((epochs, bands, slots * rows, part), BF16),
            pltpu.VMEM((epochs - 1, bands, slots * rows, part), BF16),
            pltpu.VMEM((sky - 1, bands, rows, part), BF16),
            pltpu.VMEM((bands, patch, part), F32),
            pltpu.VMEM((bands, patch, part), F32),
            pltpu.VMEM((epochs, pairs * canvas, slots * rows), BF16),
            pltpu.VMEM((epochs, bands, pairs * canvas, part), F32),
            pltpu.VMEM((epochs, bands, pairs, LANES), F32),
            pltpu.VMEM((sky - 1, bands, rows, part), BF16),
            pltpu.VMEM((sky - 1, bands, rows, part), BF16),
            pltpu.VMEM(((sky if sky <= AT_ONCE else 1) * epochs * held_slots, cols), F32),
            pltpu.SemaphoreType.DMA((bands + 2,)),
            pltpu.SemaphoreType.DMA((2,)),
            pltpu.SemaphoreType.DMA((bands,)),
            pltpu.SemaphoreType.DMA((bands + 1,)),
            pltpu.SemaphoreType.DMA((bands + 1,)),
            pltpu.SemaphoreType.DMA((5,)),
        ],
        compiler_params=pltpu.CompilerParams(collective_id=0, has_side_effects=True, vmem_limit_bytes=limit),
        name="coadd",
    )(*[
        x if x is slot_count else pltpu.with_memory_space_constraint(x, pltpu.MemorySpace.HBM)
        for x in (
            slot_count, slot_offset.T, slot_frac.T, slot_pixels, template, slot_tile.T, slot_sigma.T,
            clip_mask, prior_weight,
        )
    ])

    return pl.pallas_call(
        leave_kernel,
        out_shape=(block, block),
        in_specs=[vmem] * 2,
        out_specs=(pl.BlockSpec(memory_space=pl.ANY),) * 2,
        scratch_shapes=[pltpu.SemaphoreType.DMA((2,))],
        compiler_params=pltpu.CompilerParams(vmem_limit_bytes=1024 * 1024),
        name="leave",
    )(*results)

def solution(mesh):
    in_specs = (
        P(("groups", "sky", "epoch"), "band", None, None),
        P(("groups", "sky", "epoch"), None),
        P(("groups", "sky", "epoch"), None),
        P(("groups", "sky", "epoch"), None),
        P(("groups", "sky", "epoch"), "band"),
        P(("groups", "sky", "epoch"), None, None),
        P(("groups", "sky", "epoch")),
        P("band", ("groups", "sky"), None),
        P("band", ("groups", "sky")),
    )
    out_specs = (P("band", ("groups", "sky"), "epoch"), P("band", ("groups", "sky"), "epoch"))
    return jax.shard_map(
        on_device, mesh=mesh, in_specs=in_specs, out_specs=out_specs, check_vma=False
    )
```
